32 devices in a mesh: orb: 8 (over z, core), grp: 4 (over y, x).
Axes of the slice: x: 2, y: 2, z: 4, core: 2. Of those that a mesh axis runs over, the one named last changes fastest.
Arguments:
- orbitals: bfloat16 [512, 32, 1024], P('orb', 'grp'), may hold values from -6 to 6
- pair_list: int32 [8, 8, 3], replicated, may hold values from 0 to 63, as said below
- offsets: int32 [512, 3], replicated, may hold values from 0 to 15
Outputs:
- exchange_action: float32 [512, 32, 1024], P('orb', 'grp')
The draws below stay inside these ranges and needn't reach their ends.
Inputs may be any that keep to these rules, and one draw needn't show every extreme that they name: pair_list[o, r, 0] and pair_list[o, r, 1] are below 64; pair_list[o, r, 2] is a slot below 16, distinct within each block o, so a block names each owner group at most 2 times; in every draw some owner group is named 2 times by every block; the two orbitals of a pair differ.
All inputs are finite; a program needn't handle non-finite values.
Results may differ from the reference program's by a relative error of at most 0.0006.
Values may be sent and summed in bfloat16 or wider, within the bound.
A program may use at most 64 MiB of HBM per device.

```python
import math
import jax
import jax.numpy as jnp
from jax import lax

BOX = 32
ORB_GRP = 64
CAP = 2
ORBITALS = 512
N_ORB = 8


def draw_pair_list(key, part):
    slot_count = N_ORB * CAP
    keep_count = slot_count // 2
    base_key = jax.random.fold_in(key, 17)
    full_group = jax.random.randint(jax.random.fold_in(base_key, 1), (), 0, N_ORB)
    slot_ids = jnp.arange(slot_count, dtype=jnp.int32)

    def one_block(block_num):
        block_key = jax.random.fold_in(base_key, block_num + 100)
        key_score, key_second, key_first, key_other = jax.random.split(block_key, 4)
        scores = jax.random.randint(key_score, (slot_count,), 0, 1 << 20) * slot_count + slot_ids
        scores = jnp.where(slot_ids // CAP == full_group, -1 - slot_ids, scores)
        chosen = jnp.argsort(scores, stable=True)[:keep_count].astype(jnp.int32)
        second_local = jax.random.randint(key_second, (keep_count,), 0, ORB_GRP)
        first_raw = jax.random.randint(key_first, (keep_count,), 0, ORB_GRP)
        other_local = (second_local + 1 + jax.random.randint(key_other, (keep_count,), 0, ORB_GRP - 1)) % ORB_GRP
        first_local = jnp.where(chosen // CAP == block_num, other_local, first_raw)
        return jnp.stack([second_local, first_local, chosen], axis=1)
    return jax.vmap(one_block)(jnp.arange(N_ORB, dtype=jnp.int32)).astype(jnp.int32)


def with_ends(values, own_key, least, largest):
    longest = values.shape.index(max(values.shape))
    spots = []
    for shift in (0, 1):
        where = [jax.random.randint(jax.random.fold_in(own_key, axis), (), 0, length) for axis, length in enumerate(values.shape)]
        where[longest] = (where[longest] + shift) % values.shape[longest]
        spots.append(tuple(where))
    return values.at[spots[0]].set(least).at[spots[1]].set(largest)


def level_of(stream_key, shape, cuts, low, top_value):
    gain = 1.0
    for position, parts in cuts:
        draws = jax.random.uniform(jax.random.fold_in(jax.random.fold_in(stream_key, 6), position), (parts,), jnp.float32, low / len(cuts), top_value / len(cuts))
        gain = gain * jnp.repeat(jnp.exp(draws), shape[position] // parts).reshape((-1,) + (1,) * (len(shape) - 1 - position))
    return gain


def noise(own_key, extent, spread, reach, cuts=(), held_as=jnp.bfloat16):
    result = jax.random.normal(own_key, extent, jnp.float32) * spread
    if len(cuts) > 0:
        result = level_of(own_key, extent, cuts, -0.22, 0.18) * result
    return jnp.clip(result, min=-reach, max=reach).astype(held_as)


def setup_inputs(seed: int = 0) -> dict:
    key_of = jax.random.split(jax.random.key(seed), 4)
    orbitals = noise(key_of[0], (ORBITALS, BOX, BOX * BOX), 1.0, 6.0, ((0, 8), (1, 4)))
    pair_list = draw_pair_list(jax.random.fold_in(key_of[3], 71), 0)
    offsets = with_ends(jax.random.randint(key_of[2], (ORBITALS, 3), 0, BOX // 2), jax.random.fold_in(key_of[2], 1), 0, (BOX // 2) - 1).astype(jnp.int32)
    return {"orbitals": orbitals, "pair_list": pair_list, "offsets": offsets}


screen_shift = 0.25
highest = lax.Precision.HIGHEST
shared_forms = ('ab,pbyz->payz', 'ab,pxbz->pxaz', 'ab,pxyb->pxya')
single_forms = ('pab,pbyz->payz', 'pab,pxbz->pxaz', 'pab,pxyb->pxya')

def sine_table(length):
    counts = jnp.arange(length).astype(jnp.float32) + 1.0
    return jnp.sqrt(2.0 / (length + 1.0)) * jnp.sin(math.pi * counts[:, None] * counts[None, :] / (length + 1.0))

def green_table(length):
    counts = jnp.arange(length).astype(jnp.float32) + 1.0
    levels = 2.0 - 2.0 * jnp.cos(math.pi * counts / (length + 1.0))
    return 1.0 / (levels[:, None, None] + levels[None, :, None] + levels[None, None, :] + screen_shift)

def shift_tables(displace, length):
    places = jnp.arange(length, dtype=jnp.int32)
    return (places[None, None, :] == places[None, :, None] + displace[:, None, None]).astype(jnp.float32)

def along_shared(table, field, dimension):
    return jnp.einsum(shared_forms[dimension], table, field, precision=highest)

def along_single(tables, field, dimension):
    return jnp.einsum(single_forms[dimension], tables, field, precision=highest)

def pair_terms(first_box, second_box, displace):
    length = first_box.shape[1]
    transform = sine_table(length)
    tables = [shift_tables(displace[:, axis_num], length) for axis_num in range(3)]
    shifted = second_box
    for dimension in range(3):
        shifted = along_single(tables[dimension], shifted, dimension)
    charge = first_box * shifted
    for dimension in range(3):
        charge = along_shared(transform, charge, dimension)
    charge = charge * green_table(length)[None]
    for dimension in range(3):
        charge = along_shared(transform, charge, dimension)
    to_first = charge * shifted
    returned = charge * first_box
    for dimension in range(3):
        returned = along_single(jnp.swapaxes(tables[dimension], 1, 2), returned, dimension)
    return (to_first, returned)

def reference(orbitals, pair_list, offsets):
    length = orbitals.shape[1]
    groups = pair_list.shape[0]

    def accumulate(summed, block_data):
        block_pairs, block_num = block_data
        second_ids = (block_num * ORB_GRP + block_pairs[:, 0]).astype(jnp.int32)
        first_ids = (block_pairs[:, 2] // CAP * ORB_GRP + block_pairs[:, 1]).astype(jnp.int32)
        displace = (offsets[second_ids] - offsets[first_ids]).astype(jnp.int32)
        first_box = orbitals[first_ids].astype(jnp.float32).reshape(-1, length, length, length)
        second_box = orbitals[second_ids].astype(jnp.float32).reshape(-1, length, length, length)
        to_first, returned = pair_terms(first_box, second_box, displace)
        summed = summed.at[first_ids].add(to_first.reshape(-1, length, length * length))
        summed = summed.at[second_ids].add(returned.reshape(-1, length, length * length))
        return (summed, None)
    initial = jnp.zeros(orbitals.shape, jnp.float32)
    summed, unused = lax.scan(accumulate, initial, (pair_list, jnp.arange(groups, dtype=jnp.int32)))
    return summed
```

```python
import math

import jax
import jax.numpy as jnp
import ml_dtypes
import numpy as np
from jax import lax
from jax.experimental import pallas as pl
from jax.experimental.pallas import tpu as pltpu
from jax.sharding import PartitionSpec as P

MESH = pl.DeviceIdType.MESH
SHIFT = 0.25
F32 = jnp.float32
BF16 = jnp.bfloat16


def split_table(table):
    wide = np.asarray(table, np.float32)
    high = wide.astype(ml_dtypes.bfloat16)
    low = (wide - high.astype(np.float32)).astype(ml_dtypes.bfloat16)
    return high, low


def fixed_tables(length):
    counts = np.arange(length) + 1.0
    sine = np.sqrt(2.0 / (length + 1.0)) * np.sin(
        math.pi * counts[:, None] * counts[None, :] / (length + 1.0)
    )
    levels = 2.0 - 2.0 * np.cos(math.pi * counts / (length + 1.0))
    green = 1.0 / (
        levels[:, None, None] + levels[None, :, None] + levels[None, None, :] + SHIFT
    )
    ones = np.ones((1, length))
    return (
        np.kron(sine, ones).astype(np.float32),
        np.kron(ones, sine).astype(np.float32),
        *split_table(sine),
        green.reshape(length, length * length).astype(np.float32),
    )


def split_field(field):
    high = field.astype(BF16)
    return high, (field - high.astype(F32)).astype(BF16)


def dot(left, right):
    return jnp.dot(left, right, preferred_element_type=F32)


def ring_order(count):
    return sorted(range(1, count), key=lambda k: -min(k, count - k))


def find(pairs, block, wanted, what, rows):
    value = jnp.int32(0)
    valid = jnp.int32(0)
    for r in range(rows):
        hit = pairs[2, block, r] == wanted
        value = jnp.where(hit, jnp.int32(r) if what is None else pairs[what, block, r], value)
        valid = jnp.where(hit, jnp.int32(1), valid)
    return value, valid


def exchange_kernel(
    pairs, offsets, orbitals, outer, inner, sine_high, sine_low, green,
    landed, home,
    send_a, recv_a, stage_i, stage_j, box_i, box_j, field, shifted, second, plane_high, plane_low,
    term_i, term_j, rows_i, send_d, recv_d, rows_j,
    sem_sa, sem_ra, sem_si, sem_ri, sem_sj, sem_rj, sem_st, sem_rt, sem_su, sem_ru, sem_sd, sem_rd,
):
    groups, cap, depth, cells = send_a.shape
    regions, share = box_i.shape[:2]
    rows = regions * share
    length = regions * depth
    local_count = orbitals.shape[0]
    me = lax.axis_index("orb")
    region = lax.axis_index("grp")
    orb_steps = ring_order(groups)
    grp_steps = ring_order(regions)

    def orb_peer(k):
        return lax.rem(me + k, groups)

    def grp_peer(k):
        return lax.rem(region + k, regions)

    barrier = pltpu.get_barrier_semaphore()
    for k in orb_steps:
        pl.semaphore_signal(barrier, inc=1, device_id={"orb": orb_peer(k)}, device_id_type=MESH)
    for k in grp_steps:
        pl.semaphore_signal(barrier, inc=1, device_id={"grp": grp_peer(k)}, device_id_type=MESH)

    for block in range(groups):
        for c in range(cap):
            local, _ = find(pairs, block, me * cap + c, 1, rows)
            send_a[block, c] = orbitals[local]
    for r in range(rows):
        stage_j[r] = orbitals[pairs[0, me, r]]
    pl.semaphore_wait(barrier, groups + regions - 2)

    copies_a = []
    for k in orb_steps:
        peer = orb_peer(k)
        copy = pltpu.make_async_remote_copy(
            src_ref=send_a.at[peer], dst_ref=recv_a.at[me],
            send_sem=sem_sa.at[peer], recv_sem=sem_ra.at[me],
            device_id={"orb": peer}, device_id_type=MESH)
        copy.start()
        copies_a.append(copy)

    def grp_send(source, target, send_sem, recv_sem):
        copies = []
        for k in grp_steps:
            peer = grp_peer(k)
            copy = pltpu.make_async_remote_copy(
                src_ref=source(peer), dst_ref=target(region),
                send_sem=send_sem.at[peer], recv_sem=recv_sem.at[region],
                device_id={"grp": peer}, device_id_type=MESH)
            copy.start()
            copies.append(copy)
        return copies

    def grp_wait(source, target, send_sem, recv_sem):
        for k in grp_steps:
            peer = grp_peer(k)
            pltpu.make_async_remote_copy(
                src_ref=source(peer), dst_ref=target(peer),
                send_sem=send_sem.at[peer], recv_sem=recv_sem.at[peer],
                device_id={"grp": peer}, device_id_type=MESH).wait_recv()

    def share_rows(ref):
        return lambda part: ref.at[pl.ds(part * share, share)]

    def whole(ref):
        return lambda part: ref.at[part]

    j_args = (share_rows(stage_j), whole(box_j), sem_sj, sem_rj)
    i_args = (share_rows(stage_i), whole(box_i), sem_si, sem_ri)
    t_args = (whole(term_i), share_rows(rows_i), sem_st, sem_rt)
    u_args = (whole(term_j), share_rows(rows_j), sem_su, sem_ru)

    copies = grp_send(*j_args)
    for c in range(cap):
        recv_a[me, c] = send_a[me, c]
    for p in range(share):
        box_j[region, p] = stage_j[region * share + p]

    @pl.loop(0, length)
    def _(step):
        span = pl.ds(pl.multiple_of(step * length, length), length)
        plane_high[span, :], plane_low[span, :] = split_field(outer[pl.ds(step, 1), :] * inner[...])

    row = lax.broadcasted_iota(jnp.int32, (length, cells), 0)
    col = lax.broadcasted_iota(jnp.int32, (length, cells), 1)
    mid = col // length
    last = col - mid * length

    def shift(values, dx, dy, dz):
        moved = pltpu.roll(values, jnp.remainder(-dx + length, length), 0)
        flat = jnp.remainder(2 * cells - dy * length - dz, cells)
        moved = pltpu.roll(moved, flat, 1)
        x, y, z = row + dx, mid + dy, last + dz
        keep = (x >= 0) & (x < length) & (y >= 0) & (y < length) & (z >= 0) & (z < length)
        return jnp.where(keep, moved, 0.0)

    moves = []
    for p in range(share):
        r = region * share + p
        j = me * local_count + pairs[0, me, r]
        i = (pairs[2, me, r] // cap) * local_count + pairs[1, me, r]
        moves.append([offsets[a, j] - offsets[a, i] for a in range(3)])

    grp_wait(*j_args)
    for p in range(share):
        for part in range(regions):
            field[part * depth : (part + 1) * depth, :] = box_j[part, p].astype(F32)
        shifted[p] = shift(field[0:length, :], *moves[p])

    for k in orb_steps:
        peer = orb_peer(k)
        pltpu.make_async_remote_copy(
            src_ref=send_a.at[peer], dst_ref=recv_a.at[peer],
            send_sem=sem_sa.at[peer], recv_sem=sem_ra.at[peer],
            device_id={"orb": peer}, device_id_type=MESH).wait_recv()
    for r in range(rows):
        slot = pairs[2, me, r]
        stage_i[r] = recv_a[slot // cap, slot % cap]
    copies += grp_send(*i_args)
    for p in range(share):
        box_i[region, p] = stage_i[region * share + p]
    grp_wait(*i_args)

    for p in range(share):
        for part in range(regions):
            span = slice(part * depth, (part + 1) * depth)
            second[p, span, :] = box_i[part, p].astype(F32)
        field[p * length : (p + 1) * length, :] = second[p] * shifted[p]

    def along_plane():
        high, low = split_field(field[...])
        field[...] = (
            dot(high, plane_high[...]) + dot(low, plane_high[...]) + dot(high, plane_low[...])
        )

    def along_x(values):
        high, low = split_field(values)
        return dot(sine_high[...], high) + dot(sine_high[...], low) + dot(sine_low[...], high)

    along_plane()
    for p in range(share):
        span = slice(p * length, (p + 1) * length)
        field[span, :] = along_x(along_x(field[span, :]) * green[...])
    along_plane()
    for p in range(share):
        term = field[p * length : (p + 1) * length, :] * shifted[p]
        for part in range(regions):
            term_i[part, p] = term[part * depth : (part + 1) * depth, :]
    copies += grp_send(*t_args)
    for p in range(share):
        rows_i[region * share + p] = term_i[region, p]
        term = shift(field[p * length : (p + 1) * length, :] * second[p], *[-d for d in moves[p]])
        for part in range(regions):
            term_j[part, p] = term[part * depth : (part + 1) * depth, :]
    copies += grp_send(*u_args)
    for p in range(share):
        rows_j[region * share + p] = term_j[region, p]

    grp_wait(*t_args)
    for k in orb_steps + [0]:
        peer = orb_peer(k)
        for c in range(cap):
            r, _ = find(pairs, me, peer * cap + c, None, rows)
            send_d[peer, c] = rows_i[r]
        if k == 0:
            break
        copy = pltpu.make_async_remote_copy(
            src_ref=send_d.at[peer], dst_ref=recv_d.at[me],
            send_sem=sem_sd.at[peer], recv_sem=sem_rd.at[me],
            device_id={"orb": peer}, device_id_type=MESH)
        copy.start()
        copies_a.append(copy)
    for c in range(cap):
        recv_d[me, c] = send_d[me, c]
    grp_wait(*u_args)
    home[...] = rows_j[...]
    for k in orb_steps:
        peer = orb_peer(k)
        pltpu.make_async_remote_copy(
            src_ref=send_d.at[peer], dst_ref=recv_d.at[peer],
            send_sem=sem_sd.at[peer], recv_sem=sem_rd.at[peer],
            device_id={"orb": peer}, device_id_type=MESH).wait_recv()
    landed[...] = recv_d[...]
    for copy in copies_a + copies:
        copy.wait_send()


def exchange_terms(pairs, offsets, orbitals, groups, regions):
    _, depth, cells = orbitals.shape
    rows = pairs.shape[2]
    share = rows // regions
    cap = 2 * rows // groups
    length = depth * regions
    vmem = pl.BlockSpec(memory_space=pltpu.VMEM)
    smem = pl.BlockSpec(memory_space=pltpu.SMEM)
    by_slot = (groups, cap, depth, cells)
    by_row = (rows, depth, cells)
    by_region = (regions, share, depth, cells)
    dma = pltpu.SemaphoreType.DMA
    return pl.pallas_call(
        exchange_kernel,
        out_shape=(jax.ShapeDtypeStruct(by_slot, F32), jax.ShapeDtypeStruct(by_row, F32)),
        in_specs=[smem, smem] + [vmem] * 6,
        out_specs=(vmem, vmem),
        scratch_shapes=[
            pltpu.VMEM(by_slot, BF16), pltpu.VMEM(by_slot, BF16),
            pltpu.VMEM(by_row, BF16), pltpu.VMEM(by_row, BF16),
            pltpu.VMEM(by_region, BF16), pltpu.VMEM(by_region, BF16),
            pltpu.VMEM((share * length, cells), F32),
            pltpu.VMEM((share, length, cells), F32),
            pltpu.VMEM((share, length, cells), F32),
            pltpu.VMEM((cells, cells), BF16), pltpu.VMEM((cells, cells), BF16),
            pltpu.VMEM(by_region, F32), pltpu.VMEM(by_region, F32),
            pltpu.VMEM(by_row, F32),
            pltpu.VMEM(by_slot, F32), pltpu.VMEM(by_slot, F32),
            pltpu.VMEM(by_row, F32),
            dma((groups,)), dma((groups,)),
            dma((regions,)), dma((regions,)), dma((regions,)), dma((regions,)),
            dma((regions,)), dma((regions,)), dma((regions,)), dma((regions,)),
            dma((groups,)), dma((groups,)),
        ],
        compiler_params=pltpu.CompilerParams(
            collective_id=0, has_side_effects=True, vmem_limit_bytes=32 * 1024 * 1024),
    )(pairs, offsets, orbitals, *[jnp.asarray(t) for t in fixed_tables(length)])


def collect_kernel(pairs, landed, home, out):
    groups, cap = landed.shape[:2]
    rows = home.shape[0]
    me = lax.axis_index("orb")
    out[...] = jnp.zeros_like(out)
    for r in range(rows):
        k = pairs[0, me, r]
        out[k] += home[r]
    for block in range(groups):
        for c in range(cap):
            k, valid = find(pairs, block, me * cap + c, 1, rows)
            out[k] += jnp.where(valid > 0, landed[block, c], 0.0)


def collect(pairs, landed, home, shape):
    vmem = pl.BlockSpec(memory_space=pltpu.VMEM)
    smem = pl.BlockSpec(memory_space=pltpu.SMEM)
    return pl.pallas_call(
        collect_kernel,
        out_shape=jax.ShapeDtypeStruct(shape, F32),
        in_specs=[smem, vmem, vmem],
        out_specs=vmem,
        compiler_params=pltpu.CompilerParams(vmem_limit_bytes=32 * 1024 * 1024),
    )(pairs, landed, home)


def per_device(orbitals, pair_list, offsets):
    groups = lax.axis_size("orb")
    regions = lax.axis_size("grp")
    pairs = jnp.transpose(pair_list, (2, 0, 1))
    landed, home = exchange_terms(pairs, offsets.T, orbitals, groups, regions)
    return collect(pairs, landed, home, orbitals.shape)


def solution(mesh):
    in_specs = (P("orb", "grp", None), P(), P())
    out_specs = P("orb", "grp", None)
    return jax.shard_map(
        per_device, mesh=mesh, in_specs=in_specs, out_specs=out_specs, check_vma=False
    )
```

```python
import math

import jax
import jax.numpy as jnp
import ml_dtypes
import numpy as np
from jax import lax
from jax.experimental import pallas as pl
from jax.experimental.pallas import tpu as pltpu
from jax.sharding import PartitionSpec as P

MESH = pl.DeviceIdType.MESH
SHIFT = 0.25
LANES = 128
F32 = jnp.float32
BF16 = jnp.bfloat16


def split_table(table):
    wide = np.asarray(table, np.float32)
    high = wide.astype(ml_dtypes.bfloat16)
    low = (wide - high.astype(np.float32)).astype(ml_dtypes.bfloat16)
    return high, low


def fixed_tables(length):
    counts = np.arange(length) + 1.0
    sine = np.sqrt(2.0 / (length + 1.0)) * np.sin(
        math.pi * counts[:, None] * counts[None, :] / (length + 1.0)
    )
    levels = 2.0 - 2.0 * np.cos(math.pi * counts / (length + 1.0))
    green = 1.0 / (
        levels[:, None, None] + levels[None, :, None] + levels[None, None, :] + SHIFT
    )
    ones = np.ones((1, length))
    return (
        np.kron(sine, ones).astype(np.float32),
        np.kron(ones, sine).astype(np.float32),
        *split_table(sine),
        green.reshape(length, length * length).astype(np.float32),
    )


def split_field(field):
    high = field.astype(BF16)
    return high, (field - high.astype(F32)).astype(BF16)


def dot(left, right):
    return jnp.dot(left, right, preferred_element_type=F32)


def ring_order(count):
    return sorted(range(1, count), key=lambda k: -min(k, count - k))


def find(pairs, block, wanted, what, rows):
    value = jnp.int32(0)
    valid = jnp.int32(0)
    for r in range(rows):
        hit = pairs[2, block, r] == wanted
        value = jnp.where(hit, jnp.int32(r) if what is None else pairs[what, block, r], value)
        valid = jnp.where(hit, jnp.int32(1), valid)
    return value, valid


LEVELS = 32766.0


def encode(values):
    size = jnp.abs(values)
    top = jnp.maximum(jnp.max(jnp.max(size, axis=0, keepdims=True), axis=1, keepdims=True), 1e-36)
    steps = (jnp.sqrt(size * (1.0 / top)) * LEVELS + 0.5).astype(jnp.int32)
    code = jnp.where(values < 0.0, -steps, steps).astype(jnp.int16)
    return code, jnp.broadcast_to(top, (1, LANES))


def decode(code, top):
    steps = code.astype(jnp.int32).astype(F32)
    return steps * jnp.abs(steps) * (top[:, 0:1] * (1.0 / (LEVELS * LEVELS)))


def exchange_kernel(
    pairs_in, offsets_in, orbitals_in, outer_in, inner_in, sine_high_in, sine_low_in, green_in,
    landed, home,
    pairs, offsets, orbitals, outer, inner, sine_high, sine_low, green, sem_in,
    send_a, recv_a, stage_i, stage_j, box_i, box_j, field, shifted, second, plane_high, plane_low,
    term_i, term_j, rows_i, send_d, recv_d, rows_j, top_i, top_rows, send_top, recv_top,
    sem_sa, sem_ra, sem_si, sem_ri, sem_sj, sem_rj, sem_st, sem_rt, sem_su, sem_ru, sem_sd, sem_rd,
    sem_sv, sem_rv, sem_sw, sem_rw,
):
    groups, cap, depth, cells = send_a.shape
    regions, share = box_i.shape[:2]
    rows = regions * share
    length = regions * depth
    local_count = orbitals.shape[0]
    me = lax.axis_index("orb")
    region = lax.axis_index("grp")
    orb_steps = ring_order(groups)
    grp_steps = ring_order(regions)

    def orb_peer(k):
        return lax.rem(me + k, groups)

    def grp_peer(k):
        return lax.rem(region + k, regions)

    loads = [
        pltpu.make_async_copy(source, target, sem_in.at[n])
        for n, (source, target) in enumerate((
            (pairs_in, pairs), (orbitals_in, orbitals), (offsets_in, offsets),
            (outer_in, outer), (inner_in, inner), (green_in, green),
            (sine_high_in, sine_high), (sine_low_in, sine_low)))
    ]
    for load in loads:
        load.start()
    barrier = pltpu.get_barrier_semaphore()
    for k in orb_steps:
        pl.semaphore_signal(barrier, inc=1, device_id={"orb": orb_peer(k)}, device_id_type=MESH)
    for k in grp_steps:
        pl.semaphore_signal(barrier, inc=1, device_id={"grp": grp_peer(k)}, device_id_type=MESH)

    loads[0].wait()
    loads[1].wait()

    for block in range(groups):
        for c in range(cap):
            local, _ = find(pairs, block, me * cap + c, 1, rows)
            send_a[block, c] = orbitals[local]
    for r in range(rows):
        stage_j[r] = orbitals[pairs[0, me, r]]
    pl.semaphore_wait(barrier, groups + regions - 2)

    copies_a = []
    for k in orb_steps:
        peer = orb_peer(k)
        copy = pltpu.make_async_remote_copy(
            src_ref=send_a.at[peer], dst_ref=recv_a.at[me],
            send_sem=sem_sa.at[peer], recv_sem=sem_ra.at[me],
            device_id={"orb": peer}, device_id_type=MESH)
        copy.start()
        copies_a.append(copy)

    def grp_send(source, target, send_sem, recv_sem):
        copies = []
        for k in grp_steps:
            peer = grp_peer(k)
            copy = pltpu.make_async_remote_copy(
                src_ref=source(peer), dst_ref=target(region),
                send_sem=send_sem.at[peer], recv_sem=recv_sem.at[region],
                device_id={"grp": peer}, device_id_type=MESH)
            copy.start()
            copies.append(copy)
        return copies

    def grp_wait(source, target, send_sem, recv_sem):
        for k in grp_steps:
            peer = grp_peer(k)
            pltpu.make_async_remote_copy(
                src_ref=source(peer), dst_ref=target(peer),
                send_sem=send_sem.at[peer], recv_sem=recv_sem.at[peer],
                device_id={"grp": peer}, device_id_type=MESH).wait_recv()

    def share_rows(ref):
        return lambda part: ref.at[pl.ds(part * share, share)]

    def whole(ref):
        return lambda part: ref.at[part]

    j_args = (share_rows(stage_j), whole(box_j), sem_sj, sem_rj)
    i_args = (share_rows(stage_i), whole(box_i), sem_si, sem_ri)
    t_args = (whole(term_i), share_rows(rows_i), sem_st, sem_rt)
    v_args = (whole(top_i), whole(top_rows), sem_sv, sem_rv)
    u_args = (whole(term_j), share_rows(rows_j), sem_su, sem_ru)

    copies = grp_send(*j_args)
    for c in range(cap):
        recv_a[me, c] = send_a[me, c]
    for p in range(share):
        box_j[region, p] = stage_j[region * share + p]

    for load in loads[2:]:
        load.wait()

    @pl.loop(0, length)
    def _(step):
        span = pl.ds(pl.multiple_of(step * length, length), length)
        plane_high[span, :], plane_low[span, :] = split_field(outer[pl.ds(step, 1), :] * inner[...])

    row = lax.broadcasted_iota(jnp.int32, (length, cells), 0)
    col = lax.broadcasted_iota(jnp.int32, (length, cells), 1)
    mid = col // length
    last = col - mid * length

    def shift(values, dx, dy, dz):
        moved = pltpu.roll(values, jnp.remainder(-dx + length, length), 0)
        flat = jnp.remainder(2 * cells - dy * length - dz, cells)
        moved = pltpu.roll(moved, flat, 1)
        x, y, z = row + dx, mid + dy, last + dz
        keep = (x >= 0) & (x < length) & (y >= 0) & (y < length) & (z >= 0) & (z < length)
        return jnp.where(keep, moved, 0.0)

    moves = []
    for p in range(share):
        r = region * share + p
        j = me * local_count + pairs[0, me, r]
        i = (pairs[2, me, r] // cap) * local_count + pairs[1, me, r]
        moves.append([offsets[a, j] - offsets[a, i] for a in range(3)])

    grp_wait(*j_args)
    for p in range(share):
        for part in range(regions):
            field[part * depth : (part + 1) * depth, :] = box_j[part, p].astype(F32)
        shifted[p] = shift(field[0:length, :], *moves[p])

    for k in orb_steps:
        peer = orb_peer(k)
        pltpu.make_async_remote_copy(
            src_ref=send_a.at[peer], dst_ref=recv_a.at[peer],
            send_sem=sem_sa.at[peer], recv_sem=sem_ra.at[peer],
            device_id={"orb": peer}, device_id_type=MESH).wait_recv()
    for r in range(rows):
        slot = pairs[2, me, r]
        stage_i[r] = recv_a[slot // cap, slot % cap]
    copies += grp_send(*i_args)
    for p in range(share):
        box_i[region, p] = stage_i[region * share + p]
    grp_wait(*i_args)

    for p in range(share):
        for part in range(regions):
            span = slice(part * depth, (part + 1) * depth)
            second[p, span, :] = box_i[part, p].astype(F32)
        field[p * length : (p + 1) * length, :] = second[p] * shifted[p]

    def along_plane():
        high, low = split_field(field[...])
        field[...] = (
            dot(high, plane_high[...]) + dot(low, plane_high[...]) + dot(high, plane_low[...])
        )

    def along_x(values):
        high, low = split_field(values)
        return dot(sine_high[...], high) + dot(sine_high[...], low) + dot(sine_low[...], high)

    along_plane()
    for p in range(share):
        span = slice(p * length, (p + 1) * length)
        field[span, :] = along_x(along_x(field[span, :]) * green[...])
    along_plane()
    for p in range(share):
        code, top = encode(field[p * length : (p + 1) * length, :] * shifted[p])
        for part in range(regions):
            term_i[part, p] = code[part * depth : (part + 1) * depth, :]
            top_i[part, p : p + 1] = top
    copies += grp_send(*t_args)
    copies += grp_send(*v_args)
    for p in range(share):
        rows_i[region * share + p] = term_i[region, p]
    top_rows[region] = top_i[region]
    for p in range(share):
        term = shift(field[p * length : (p + 1) * length, :] * second[p], *[-d for d in moves[p]])
        for part in range(regions):
            term_j[part, p] = term[part * depth : (part + 1) * depth, :]
    copies += grp_send(*u_args)
    for p in range(share):
        rows_j[region * share + p] = term_j[region, p]

    grp_wait(*t_args)
    grp_wait(*v_args)
    for peer in range(groups):
        for c in range(cap):
            r, _ = find(pairs, me, peer * cap + c, None, rows)
            send_d[peer, c] = rows_i[r]
            send_top[peer, c : c + 1] = top_rows[r // share, pl.ds(r % share, 1)]

    d_args = (send_d, recv_d, sem_sd, sem_rd)
    w_args = (send_top, recv_top, sem_sw, sem_rw)

    def orb_copy(k, arriving, source, target, send_sem, recv_sem):
        peer = orb_peer(k)
        place = peer if arriving else me
        return pltpu.make_async_remote_copy(
            src_ref=source.at[peer], dst_ref=target.at[place],
            send_sem=send_sem.at[peer], recv_sem=recv_sem.at[place],
            device_id={"orb": peer}, device_id_type=MESH)

    for k in orb_steps:
        for args in (w_args, d_args):
            copy = orb_copy(k, False, *args)
            copy.start()
            copies_a.append(copy)

    def arrived(source, codes, tops):
        for c in range(cap):
            landed[source, c] = decode(codes[source, c], tops[source, c : c + 1])

    arrived(me, send_d, send_top)
    grp_wait(*u_args)
    home[...] = rows_j[...]
    for k in orb_steps[::-1]:
        for args in (w_args, d_args):
            orb_copy(k, True, *args).wait_recv()
        arrived(orb_peer(k), recv_d, recv_top)
    for copy in copies_a + copies:
        copy.wait_send()


def exchange_terms(pairs, offsets, orbitals, groups, regions):
    _, depth, cells = orbitals.shape
    rows = pairs.shape[2]
    share = rows // regions
    cap = 2 * rows // groups
    length = depth * regions
    vmem = pl.BlockSpec(memory_space=pltpu.VMEM)
    tables = [jnp.asarray(t) for t in fixed_tables(length)]
    operands = (pairs, offsets, orbitals, *tables)
    spaces = [pltpu.SMEM, pltpu.SMEM] + [pltpu.VMEM] * 6
    by_slot = (groups, cap, depth, cells)
    by_row = (rows, depth, cells)
    by_region = (regions, share, depth, cells)
    dma = pltpu.SemaphoreType.DMA
    return pl.pallas_call(
        exchange_kernel,
        out_shape=(jax.ShapeDtypeStruct(by_slot, F32), jax.ShapeDtypeStruct(by_row, F32)),
        in_specs=[pl.BlockSpec(memory_space=pltpu.HBM)] * 8,
        out_specs=(vmem, vmem),
        scratch_shapes=[
            *[space(x.shape, x.dtype) for space, x in zip(spaces, operands)],
            dma((len(operands),)),
            pltpu.VMEM(by_slot, BF16), pltpu.VMEM(by_slot, BF16),
            pltpu.VMEM(by_row, BF16), pltpu.VMEM(by_row, BF16),
            pltpu.VMEM(by_region, BF16), pltpu.VMEM(by_region, BF16),
            pltpu.VMEM((share * length, cells), F32),
            pltpu.VMEM((share, length, cells), F32),
            pltpu.VMEM((share, length, cells), F32),
            pltpu.VMEM((cells, cells), BF16), pltpu.VMEM((cells, cells), BF16),
            pltpu.VMEM(by_region, jnp.int16), pltpu.VMEM(by_region, F32),
            pltpu.VMEM(by_row, jnp.int16),
            pltpu.VMEM(by_slot, jnp.int16), pltpu.VMEM(by_slot, jnp.int16),
            pltpu.VMEM(by_row, F32),
            pltpu.VMEM((regions, share, LANES), F32), pltpu.VMEM((regions, share, LANES), F32),
            pltpu.VMEM((groups, cap, LANES), F32), pltpu.VMEM((groups, cap, LANES), F32),
            dma((groups,)), dma((groups,)),
            dma((regions,)), dma((regions,)), dma((regions,)), dma((regions,)),
            dma((regions,)), dma((regions,)), dma((regions,)), dma((regions,)),
            dma((groups,)), dma((groups,)),
            dma((regions,)), dma((regions,)), dma((groups,)), dma((groups,)),
        ],
        compiler_params=pltpu.CompilerParams(
            collective_id=0, has_side_effects=True, vmem_limit_bytes=32 * 1024 * 1024),
    )(*[pltpu.with_memory_space_constraint(x, pltpu.HBM) for x in operands])


def collect_kernel(pairs_in, landed, home, out, pairs, sem_in):
    groups, cap = landed.shape[:2]
    rows = home.shape[0]
    me = lax.axis_index("orb")
    load = pltpu.make_async_copy(pairs_in, pairs, sem_in)
    load.start()
    out[...] = jnp.zeros_like(out)
    load.wait()
    for r in range(rows):
        k = pairs[0, me, r]
        out[k] += home[r]
    for block in range(groups):
        for c in range(cap):
            k, valid = find(pairs, block, me * cap + c, 1, rows)
            out[k] += jnp.where(valid > 0, landed[block, c], 0.0)


def collect(pairs, landed, home, shape):
    vmem = pl.BlockSpec(memory_space=pltpu.VMEM)
    return pl.pallas_call(
        collect_kernel,
        out_shape=jax.ShapeDtypeStruct(shape, F32),
        in_specs=[pl.BlockSpec(memory_space=pltpu.HBM), vmem, vmem],
        out_specs=vmem,
        scratch_shapes=[pltpu.SMEM(pairs.shape, pairs.dtype), pltpu.SemaphoreType.DMA],
        compiler_params=pltpu.CompilerParams(vmem_limit_bytes=32 * 1024 * 1024),
    )(pltpu.with_memory_space_constraint(pairs, pltpu.HBM), landed, home)


def per_device(orbitals, pair_list, offsets):
    groups = lax.axis_size("orb")
    regions = lax.axis_size("grp")
    pairs = jnp.transpose(pair_list, (2, 0, 1))
    landed, home = exchange_terms(pairs, offsets.T, orbitals, groups, regions)
    return collect(pairs, landed, home, orbitals.shape)


def solution(mesh):
    in_specs = (P("orb", "grp", None), P(), P())
    out_specs = P("orb", "grp", None)
    return jax.shard_map(
        per_device, mesh=mesh, in_specs=in_specs, out_specs=out_specs, check_vma=False
    )
```

```python
import math

import jax
import jax.numpy as jnp
import ml_dtypes
import numpy as np
from jax import lax
from jax.experimental import pallas as pl
from jax.experimental.pallas import tpu as pltpu
from jax.sharding import PartitionSpec as P

MESH = pl.DeviceIdType.MESH
SHIFT = 0.25
LANES = 128
F32 = jnp.float32
BF16 = jnp.bfloat16


def split_table(table):
    wide = np.asarray(table, np.float32)
    high = wide.astype(ml_dtypes.bfloat16)
    low = (wide - high.astype(np.float32)).astype(ml_dtypes.bfloat16)
    return high, low


def fixed_tables(length):
    counts = np.arange(length) + 1.0
    sine = np.sqrt(2.0 / (length + 1.0)) * np.sin(
        math.pi * counts[:, None] * counts[None, :] / (length + 1.0)
    )
    levels = 2.0 - 2.0 * np.cos(math.pi * counts / (length + 1.0))
    green = 1.0 / (
        levels[:, None, None] + levels[None, :, None] + levels[None, None, :] + SHIFT
    )
    half = length // 2
    parity = np.concatenate([np.arange(0, length, 2), np.arange(1, length, 2)])
    ones = np.ones((1, length))
    near = [sine[:half, rows] for rows in (parity[:half], parity[half:])]
    outer = np.stack([np.kron(part, ones) for part in (near[0], near[1], near[0].T, near[1].T)])
    high, low = split_table(sine)
    return (
        outer.astype(np.float32),
        np.kron(np.ones((1, half)), sine).astype(np.float32),
        np.concatenate([high, high, low], axis=1),
        green[:, parity].reshape(length, length * length).astype(np.float32),
    )


def split_field(field):
    high = field.astype(BF16)
    return high, (field - high.astype(F32)).astype(BF16)


def dot(left, right):
    return jnp.dot(left, right, preferred_element_type=F32)


def ring_order(count):
    return sorted(range(1, count), key=lambda k: -min(k, count - k))


def find(pairs, block, wanted, what, rows):
    value = jnp.int32(0)
    valid = jnp.int32(0)
    for r in range(rows):
        hit = pairs[2, block, r] == wanted
        value = jnp.where(hit, jnp.int32(r) if what is None else pairs[what, block, r], value)
        valid = jnp.where(hit, jnp.int32(1), valid)
    return value, valid


LEVELS = 32766.0


def encode(values):
    size = jnp.abs(values)
    top = jnp.maximum(jnp.max(jnp.max(size, axis=0, keepdims=True), axis=1, keepdims=True), 1e-36)
    steps = (jnp.sqrt(size * (1.0 / top)) * LEVELS + 0.5).astype(jnp.int32)
    code = jnp.where(values < 0.0, -steps, steps).astype(jnp.int16)
    return code, jnp.broadcast_to(top, (1, LANES))


def decode(code, top):
    steps = code.astype(jnp.int32).astype(F32)
    return steps * jnp.abs(steps) * (top[:, 0:1] * (1.0 / (LEVELS * LEVELS)))


def exchange_kernel(
    pairs_in, offsets_in, orbitals_in, outer_in, inner_in, sine_in, green_in,
    landed, home,
    pairs, offsets, orbitals, outer, inner, sine, green, sem_in,
    send_a, recv_a, stage_i, stage_j, box_i, box_j, field, shifted, second, plane_high, plane_low,
    term_i, term_j, rows_i, send_d, recv_d, rows_j, top_i, top_rows, send_top, recv_top,
    sem_sa, sem_ra, sem_si, sem_ri, sem_sj, sem_rj, sem_st, sem_rt, sem_su, sem_ru, sem_sd, sem_rd,
    sem_sv, sem_rv, sem_sw, sem_rw,
):
    groups, cap, depth, cells = send_a.shape
    regions, share = box_i.shape[:2]
    rows = regions * share
    length = regions * depth
    local_count = orbitals.shape[0]
    me = lax.axis_index("orb")
    region = lax.axis_index("grp")
    orb_steps = ring_order(groups)
    grp_steps = ring_order(regions)

    def orb_peer(k):
        return lax.rem(me + k, groups)

    def grp_peer(k):
        return lax.rem(region + k, regions)

    loads = [
        pltpu.make_async_copy(source, target, sem_in.at[n])
        for n, (source, target) in enumerate((
            (pairs_in, pairs), (orbitals_in, orbitals), (offsets_in, offsets),
            (outer_in, outer), (inner_in, inner), (green_in, green), (sine_in, sine)))
    ]
    for load in loads:
        load.start()
    barrier = pltpu.get_barrier_semaphore()
    for k in orb_steps:
        pl.semaphore_signal(barrier, inc=1, device_id={"orb": orb_peer(k)}, device_id_type=MESH)
    for k in grp_steps:
        pl.semaphore_signal(barrier, inc=1, device_id={"grp": grp_peer(k)}, device_id_type=MESH)

    loads[0].wait()
    loads[1].wait()

    for block in range(groups):
        for c in range(cap):
            local, _ = find(pairs, block, me * cap + c, 1, rows)
            send_a[block, c] = orbitals[local]
    for r in range(rows):
        stage_j[r] = orbitals[pairs[0, me, r]]
    pl.semaphore_wait(barrier, groups + regions - 2)

    copies_a = []
    for k in orb_steps:
        peer = orb_peer(k)
        copy = pltpu.make_async_remote_copy(
            src_ref=send_a.at[peer], dst_ref=recv_a.at[me],
            send_sem=sem_sa.at[peer], recv_sem=sem_ra.at[me],
            device_id={"orb": peer}, device_id_type=MESH)
        copy.start()
        copies_a.append(copy)

    def grp_send(source, target, send_sem, recv_sem):
        copies = []
        for k in grp_steps:
            peer = grp_peer(k)
            copy = pltpu.make_async_remote_copy(
                src_ref=source(peer), dst_ref=target(region),
                send_sem=send_sem.at[peer], recv_sem=recv_sem.at[region],
                device_id={"grp": peer}, device_id_type=MESH)
            copy.start()
            copies.append(copy)
        return copies

    def grp_wait(source, target, send_sem, recv_sem):
        for k in grp_steps:
            peer = grp_peer(k)
            pltpu.make_async_remote_copy(
                src_ref=source(peer), dst_ref=target(peer),
                send_sem=send_sem.at[peer], recv_sem=recv_sem.at[peer],
                device_id={"grp": peer}, device_id_type=MESH).wait_recv()

    def share_rows(ref):
        return lambda part: ref.at[pl.ds(part * share, share)]

    def whole(ref):
        return lambda part: ref.at[part]

    j_args = (share_rows(stage_j), whole(box_j), sem_sj, sem_rj)
    i_args = (share_rows(stage_i), whole(box_i), sem_si, sem_ri)
    t_args = (whole(term_i), share_rows(rows_i), sem_st, sem_rt)
    v_args = (whole(top_i), whole(top_rows), sem_sv, sem_rv)
    u_args = (whole(term_j), share_rows(rows_j), sem_su, sem_ru)

    copies = grp_send(*j_args)
    for c in range(cap):
        recv_a[me, c] = send_a[me, c]
    for p in range(share):
        box_j[region, p] = stage_j[region * share + p]

    for load in loads[2:]:
        load.wait()

    half = length // 2

    @pl.loop(0, half)
    def _(step):
        span = pl.ds(pl.multiple_of(step * length, length), length)
        for n in range(4):
            plane_high[n, span, :], plane_low[n, span, :] = split_field(
                outer[n, pl.ds(step, 1), :] * inner[...])

    row = lax.broadcasted_iota(jnp.int32, (length, cells), 0)
    col = lax.broadcasted_iota(jnp.int32, (length, cells), 1)
    mid = col // length
    last = col - mid * length

    def shift(values, dx, dy, dz):
        moved = pltpu.roll(values, jnp.remainder(-dx + length, length), 0)
        flat = jnp.remainder(2 * cells - dy * length - dz, cells)
        moved = pltpu.roll(moved, flat, 1)
        x, y, z = row + dx, mid + dy, last + dz
        keep = (x >= 0) & (x < length) & (y >= 0) & (y < length) & (z >= 0) & (z < length)
        return jnp.where(keep, moved, 0.0)

    moves = []
    for p in range(share):
        r = region * share + p
        j = me * local_count + pairs[0, me, r]
        i = (pairs[2, me, r] // cap) * local_count + pairs[1, me, r]
        moves.append([offsets[a, j] - offsets[a, i] for a in range(3)])

    grp_wait(*j_args)
    for p in range(share):
        for part in range(regions):
            field[part * depth : (part + 1) * depth, :] = box_j[part, p].astype(F32)
        shifted[p] = shift(field[0:length, :], *moves[p])

    for k in orb_steps:
        peer = orb_peer(k)
        pltpu.make_async_remote_copy(
            src_ref=send_a.at[peer], dst_ref=recv_a.at[peer],
            send_sem=sem_sa.at[peer], recv_sem=sem_ra.at[peer],
            device_id={"orb": peer}, device_id_type=MESH).wait_recv()
    for r in range(rows):
        slot = pairs[2, me, r]
        stage_i[r] = recv_a[slot // cap, slot % cap]
    copies += grp_send(*i_args)
    for p in range(share):
        box_i[region, p] = stage_i[region * share + p]
    grp_wait(*i_args)

    for p in range(share):
        for part in range(regions):
            span = slice(part * depth, (part + 1) * depth)
            second[p, span, :] = box_i[part, p].astype(F32)
        field[p * length : (p + 1) * length, :] = second[p] * shifted[p]

    flip = lax.rem(lax.broadcasted_iota(jnp.int32, (share * length, LANES), 1) // length, 2) == 0

    def mirrored(values):
        tiles = []
        for n in range(values.shape[1] // LANES)[::-1]:
            tile = values[:, n * LANES : (n + 1) * LANES]
            tiles.append(jnp.where(flip, pltpu.roll(tile, length, 1), pltpu.roll(tile, LANES - length, 1)))
        return jnp.concatenate(tiles, axis=1)

    def product(values, n):
        count = values.shape[0]
        high, low = split_field(values)
        both = dot(jnp.concatenate([high, low], axis=0), plane_high[n])
        return both[:count] + both[count:] + dot(high, plane_low[n])

    def along_x(values):
        high, low = split_field(values)
        return dot(sine[...], jnp.concatenate([high, low, high], axis=0))

    middle = cells // 2
    near, far = field[:, :middle], mirrored(field[:, middle:])
    field[:, :middle] = product(near + far, 0)
    field[:, middle:] = product(near - far, 1)
    for p in range(share):
        span = slice(p * length, (p + 1) * length)
        field[span, :] = along_x(along_x(field[span, :]) * green[...])
    even = product(field[:, :middle], 2)
    odd = product(field[:, middle:], 3)
    field[:, :middle] = even + odd
    field[:, middle:] = mirrored(even - odd)
    for p in range(share):
        code, top = encode(field[p * length : (p + 1) * length, :] * shifted[p])
        for part in range(regions):
            term_i[part, p] = code[part * depth : (part + 1) * depth, :]
            top_i[part, p : p + 1] = top
    copies += grp_send(*t_args)
    copies += grp_send(*v_args)
    for p in range(share):
        rows_i[region * share + p] = term_i[region, p]
    top_rows[region] = top_i[region]
    for p in range(share):
        term = shift(field[p * length : (p + 1) * length, :] * second[p], *[-d for d in moves[p]])
        for part in range(regions):
            term_j[part, p] = term[part * depth : (part + 1) * depth, :]
    for p in range(share):
        rows_j[region * share + p] = term_j[region, p]

    grp_wait(*t_args)
    grp_wait(*v_args)
    for peer in range(groups):
        for c in range(cap):
            r, _ = find(pairs, me, peer * cap + c, None, rows)
            send_d[peer, c] = rows_i[r]
            send_top[peer, c : c + 1] = top_rows[r // share, pl.ds(r % share, 1)]

    d_args = (send_d, recv_d, sem_sd, sem_rd)
    w_args = (send_top, recv_top, sem_sw, sem_rw)

    def orb_copy(k, arriving, source, target, send_sem, recv_sem):
        peer = orb_peer(k)
        place = peer if arriving else me
        return pltpu.make_async_remote_copy(
            src_ref=source.at[peer], dst_ref=target.at[place],
            send_sem=send_sem.at[peer], recv_sem=recv_sem.at[place],
            device_id={"orb": peer}, device_id_type=MESH)

    for k in orb_steps:
        for args in (w_args, d_args):
            copy = orb_copy(k, False, *args)
            copy.start()
            copies_a.append(copy)

    copies += grp_send(*u_args)

    def arrived(source, codes, tops):
        for c in range(cap):
            landed[source, c] = decode(codes[source, c], tops[source, c : c + 1])

    arrived(me, send_d, send_top)
    grp_wait(*u_args)
    home[...] = rows_j[...]
    for k in orb_steps[::-1]:
        for args in (w_args, d_args):
            orb_copy(k, True, *args).wait_recv()
        arrived(orb_peer(k), recv_d, recv_top)
    for copy in copies_a + copies:
        copy.wait_send()


def exchange_terms(pairs, offsets, orbitals, groups, regions):
    _, depth, cells = orbitals.shape
    rows = pairs.shape[2]
    share = rows // regions
    cap = 2 * rows // groups
    length = depth * regions
    vmem = pl.BlockSpec(memory_space=pltpu.VMEM)
    tables = [jnp.asarray(t) for t in fixed_tables(length)]
    operands = (pairs, offsets, orbitals, *tables)
    spaces = [pltpu.SMEM, pltpu.SMEM] + [pltpu.VMEM] * 5
    by_slot = (groups, cap, depth, cells)
    by_row = (rows, depth, cells)
    by_region = (regions, share, depth, cells)
    dma = pltpu.SemaphoreType.DMA
    return pl.pallas_call(
        exchange_kernel,
        out_shape=(jax.ShapeDtypeStruct(by_slot, F32), jax.ShapeDtypeStruct(by_row, F32)),
        in_specs=[pl.BlockSpec(memory_space=pltpu.HBM)] * 7,
        out_specs=(vmem, vmem),
        scratch_shapes=[
            *[space(x.shape, x.dtype) for space, x in zip(spaces, operands)],
            dma((len(operands),)),
            pltpu.VMEM(by_slot, BF16), pltpu.VMEM(by_slot, BF16),
            pltpu.VMEM(by_row, BF16), pltpu.VMEM(by_row, BF16),
            pltpu.VMEM(by_region, BF16), pltpu.VMEM(by_region, BF16),
            pltpu.VMEM((share * length, cells), F32),
            pltpu.VMEM((share, length, cells), F32),
            pltpu.VMEM((share, length, cells), F32),
            pltpu.VMEM((4, cells // 2, cells // 2), BF16), pltpu.VMEM((4, cells // 2, cells // 2), BF16),
            pltpu.VMEM(by_region, jnp.int16), pltpu.VMEM(by_region, F32),
            pltpu.VMEM(by_row, jnp.int16),
            pltpu.VMEM(by_slot, jnp.int16), pltpu.VMEM(by_slot, jnp.int16),
            pltpu.VMEM(by_row, F32),
            pltpu.VMEM((regions, share, LANES), F32), pltpu.VMEM((regions, share, LANES), F32),
            pltpu.VMEM((groups, cap, LANES), F32), pltpu.VMEM((groups, cap, LANES), F32),
            dma((groups,)), dma((groups,)),
            dma((regions,)), dma((regions,)), dma((regions,)), dma((regions,)),
            dma((regions,)), dma((regions,)), dma((regions,)), dma((regions,)),
            dma((groups,)), dma((groups,)),
            dma((regions,)), dma((regions,)), dma((groups,)), dma((groups,)),
        ],
        compiler_params=pltpu.CompilerParams(
            collective_id=0, has_side_effects=True, vmem_limit_bytes=32 * 1024 * 1024),
    )(*[pltpu.with_memory_space_constraint(x, pltpu.HBM) for x in operands])


def collect_kernel(pairs_in, landed, home, out, pairs, sem_in):
    groups, cap = landed.shape[:2]
    rows = home.shape[0]
    me = lax.axis_index("orb")
    load = pltpu.make_async_copy(pairs_in, pairs, sem_in)
    load.start()
    out[...] = jnp.zeros_like(out)
    load.wait()
    for r in range(rows):
        k = pairs[0, me, r]
        out[k] += home[r]
    for block in range(groups):
        for c in range(cap):
            k, valid = find(pairs, block, me * cap + c, 1, rows)
            out[k] += jnp.where(valid > 0, landed[block, c], 0.0)


def collect(pairs, landed, home, shape):
    vmem = pl.BlockSpec(memory_space=pltpu.VMEM)
    return pl.pallas_call(
        collect_kernel,
        out_shape=jax.ShapeDtypeStruct(shape, F32),
        in_specs=[pl.BlockSpec(memory_space=pltpu.HBM), vmem, vmem],
        out_specs=vmem,
        scratch_shapes=[pltpu.SMEM(pairs.shape, pairs.dtype), pltpu.SemaphoreType.DMA],
        compiler_params=pltpu.CompilerParams(vmem_limit_bytes=32 * 1024 * 1024),
    )(pltpu.with_memory_space_constraint(pairs, pltpu.HBM), landed, home)


def per_device(orbitals, pair_list, offsets):
    groups = lax.axis_size("orb")
    regions = lax.axis_size("grp")
    pairs = jnp.transpose(pair_list, (2, 0, 1))
    landed, home = exchange_terms(pairs, offsets.T, orbitals, groups, regions)
    return collect(pairs, landed, home, orbitals.shape)


def solution(mesh):
    in_specs = (P("orb", "grp", None), P(), P())
    out_specs = P("orb", "grp", None)
    return jax.shard_map(
        per_device, mesh=mesh, in_specs=in_specs, out_specs=out_specs, check_vma=False
    )
```

```python
import math

import jax
import jax.numpy as jnp
import ml_dtypes
import numpy as np
from jax import lax
from jax.experimental import pallas as pl
from jax.experimental.pallas import tpu as pltpu
from jax.sharding import PartitionSpec as P

MESH = pl.DeviceIdType.MESH
SHIFT = 0.25
LANES = 128
F32 = jnp.float32
BF16 = jnp.bfloat16


def split_table(table):
    wide = np.asarray(table, np.float32)
    high = wide.astype(ml_dtypes.bfloat16)
    low = (wide - high.astype(np.float32)).astype(ml_dtypes.bfloat16)
    return high, low


def fixed_tables(length):
    counts = np.arange(length) + 1.0
    sine = np.sqrt(2.0 / (length + 1.0)) * np.sin(
        math.pi * counts[:, None] * counts[None, :] / (length + 1.0)
    )
    levels = 2.0 - 2.0 * np.cos(math.pi * counts / (length + 1.0))
    green = 1.0 / (
        levels[:, None, None] + levels[None, :, None] + levels[None, None, :] + SHIFT
    )
    half = length // 2
    parity = np.concatenate([np.arange(0, length, 2), np.arange(1, length, 2)])
    ones = np.ones((1, length))
    near = [sine[:half, rows] for rows in (parity[:half], parity[half:])]
    outer = np.stack([np.kron(part, ones) for part in (near[0], near[1], near[0].T, near[1].T)])
    high, low = split_table(sine)
    width = half * length
    inner = np.kron(np.ones((1, half)), sine)
    wide = np.zeros((length, width))
    wide[:, : 3 * length] = np.concatenate([high, high, low], axis=1).astype(np.float32)
    green = green[:, parity].reshape(length, 2 * width)
    return np.concatenate(
        [outer.reshape(4 * half, width), inner, wide, green[:, :width], green[:, width:]]
    ).astype(np.float32)


def split_field(field):
    high = field.astype(BF16)
    return high, (field - high.astype(F32)).astype(BF16)


def dot(left, right):
    return jnp.dot(left, right, preferred_element_type=F32)


def grp_order(count):
    return sorted(range(1, count), key=lambda k: -min(k, count - k))


def slot_order(groups, cap, regions, rows):
    far = list(range(groups))[::-1]
    share = rows // regions
    needed = [((b + 1) * regions - 1 + groups * cap - rows) // cap + 1 for b in range(share)]
    closed = [(b + 1) * regions // cap for b in range(share - 1)] + [groups]
    late, early = groups - needed[0], closed[0]
    order = far[:early] + far[early + late :] + far[early : early + late]
    return order, needed, closed


def partner(index, offset):
    value, bit = index, 1
    while bit <= offset:
        if offset & bit:
            value = value + bit - 2 * bit * lax.rem(lax.div(index, bit), 2)
        bit *= 2
    return value


def find(pairs, block, wanted, what, rows):
    value = jnp.int32(0)
    valid = jnp.int32(0)
    for r in range(rows):
        hit = pairs[2, block, r] == wanted
        value = jnp.where(hit, what(r), value)
        valid = jnp.where(hit, jnp.int32(1), valid)
    return value, valid


LEVELS = 32766.0


def encode(values):
    size = jnp.abs(values)
    top = jnp.maximum(jnp.max(jnp.max(size, axis=0, keepdims=True), axis=1, keepdims=True), 1e-36)
    steps = (jnp.sqrt(size * (1.0 / top)) * LEVELS + 0.5).astype(jnp.int32)
    code = jnp.where(values < 0.0, -steps, steps).astype(jnp.int16)
    return code, jnp.broadcast_to(top, (1, LANES))


def decode(code, top):
    steps = code.astype(jnp.int32).astype(F32)
    return steps * jnp.abs(steps) * (top[:, 0:1] * (1.0 / (LEVELS * LEVELS)))


def exchange_kernel(
    pairs_in, offsets_in, orbitals_in, tables_in,
    landed, home,
    pairs, offsets, orbitals, tables, sem_in,
    send_a, recv_a, slots_a, stage_i, stage_j, box_i, box_j, field, shifted, second,
    plane_high, plane_low, term_i, term_j, rows_i, every_i, rows_j, top_i, top_rows, every_top,
    send_d, recv_d, send_top, recv_top,
    sem_sa, sem_ra, sem_si, sem_ri, sem_sj, sem_rj, sem_st, sem_rt, sem_su, sem_ru, sem_sd, sem_rd,
    sem_sv, sem_rv, sem_sw, sem_rw,
):
    groups, cap, depth, cells = send_a.shape
    share, regions = box_i.shape[:2]
    rows = regions * share
    length = regions * depth
    local_count = orbitals.shape[0]
    me = lax.axis_index("orb")
    region = lax.axis_index("grp")
    grp_steps = grp_order(regions)
    order, needed, closed = slot_order(groups, cap, regions, rows)
    batches = range(share)
    begun = []

    def grp_peer(k):
        return lax.rem(region + k, regions)

    def other(n):
        return partner(me, order[n])

    loads = [
        pltpu.make_async_copy(source, target, sem_in.at[n])
        for n, (source, target) in enumerate((
            (pairs_in, pairs), (orbitals_in, orbitals), (offsets_in, offsets),
            (tables_in, tables)))
    ]
    for load in loads:
        load.start()
    barrier = pltpu.get_barrier_semaphore()
    for k in range(1, groups):
        pl.semaphore_signal(
            barrier, inc=1, device_id={"orb": lax.rem(me + k, groups)}, device_id_type=MESH)
    for k in grp_steps:
        pl.semaphore_signal(barrier, inc=1, device_id={"grp": grp_peer(k)}, device_id_type=MESH)
    loads[0].wait()

    places = []
    for r in range(rows):
        slot = pairs[2, me, r]
        group = lax.div(slot, cap)
        place = jnp.int32(0)
        for n in range(groups):
            place = jnp.where(group == other(n), jnp.int32(n * cap), place)
        places.append(place + lax.rem(slot, cap))
    ranks = []
    for r in range(rows):
        rank = jnp.int32(0)
        for q in range(rows):
            if q != r:
                rank = rank + jnp.where(places[q] < places[r], jnp.int32(1), jnp.int32(0))
        ranks.append(rank)

    def ranked(values, rank):
        value = jnp.int32(0)
        for r in range(rows):
            value = jnp.where(ranks[r] == rank, values[r], value)
        return value

    row_of = [ranked([jnp.int32(r) for r in range(rows)], q) for q in range(rows)]
    place_of = [ranked(places, q) for q in range(rows)]

    asked = []
    for n in range(groups):
        block = other(n)
        for c in range(cap):
            asked.append(find(pairs, block, me * cap + c, lambda r: pairs[1, block, r], rows)[0])
    loads[1].wait()
    for n in range(groups):
        for c in range(cap):
            send_a[n, c] = orbitals[asked[n * cap + c]]
    for b in batches:
        for part in range(regions):
            stage_j[part, b] = orbitals[pairs[0, me, row_of[b * regions + part]]]
    pl.semaphore_wait(barrier, groups + regions - 2)

    def orb_copy(n, source, target, send_sem, recv_sem):
        return pltpu.make_async_remote_copy(
            src_ref=source, dst_ref=target, send_sem=send_sem, recv_sem=recv_sem,
            device_id={"orb": other(n)}, device_id_type=MESH)

    def bytes_of(ref, sem):
        return pltpu.make_async_copy(ref, ref, sem)

    def grp_send(source, target, send_sem, recv_sem):
        for k in grp_steps:
            peer = grp_peer(k)
            pltpu.make_async_remote_copy(
                src_ref=source.at[peer], dst_ref=target.at[region],
                send_sem=send_sem, recv_sem=recv_sem,
                device_id={"grp": peer}, device_id_type=MESH).start()
        begun.append(bytes_of(source.at[pl.ds(0, regions - 1)], send_sem))

    def grp_wait(source, target, send_sem, recv_sem):
        bytes_of(target.at[pl.ds(0, regions - 1)], recv_sem).wait()

    j_args = (stage_j, box_j, sem_sj.at[0], sem_rj.at[0])
    i_args = [(stage_i.at[b], box_i.at[b], sem_si.at[b], sem_ri.at[b]) for b in batches]
    t_args = [(term_i.at[b], rows_i[b], sem_st.at[b], sem_rt.at[b]) for b in batches]
    v_args = [(top_i.at[b], top_rows[b], sem_sv.at[b], sem_rv.at[b]) for b in batches]
    u_args = [(term_j.at[b], rows_j.at[b], sem_su.at[b], sem_ru.at[b]) for b in batches]

    spans = [range(needed[b - 1] if b else 0, needed[b]) for b in batches]

    def box_copy(b, n):
        return orb_copy(n, send_a.at[n], recv_a[b].at[n - spans[b][0]], sem_sa.at[0], sem_ra.at[b])

    for b in batches:
        for n in spans[b]:
            if order[n]:
                box_copy(b, n).start()
    begun.append(bytes_of(send_a.at[pl.ds(0, groups - 1)], sem_sa.at[0]))
    grp_send(*j_args)
    for b in batches:
        for n in spans[b]:
            if not order[n]:
                for c in range(cap):
                    recv_a[b][n - spans[b][0], c] = send_a[n, c]
    box_j[region] = stage_j[region]

    for load in loads[2:]:
        load.wait()
    half = length // 2
    inner, wide, near, far = [
        slice(4 * half + n * length, 4 * half + (n + 1) * length) for n in range(4)]

    @pl.loop(0, half)
    def _(step):
        span = pl.ds(pl.multiple_of(step * length, length), length)
        for n in range(4):
            plane_high[n, span, :], plane_low[n, span, :] = split_field(
                tables[pl.ds(n * half + step, 1), :] * tables[inner, :])

    sine = tables[wide, : 3 * length].astype(BF16)
    green = jnp.concatenate([tables[near, :], tables[far, :]], axis=1)

    row = lax.broadcasted_iota(jnp.int32, (length, cells), 0)
    col = lax.broadcasted_iota(jnp.int32, (length, cells), 1)
    mid = col // length
    last = col - mid * length
    flip = lax.rem(lax.broadcasted_iota(jnp.int32, (length, LANES), 1) // length, 2) == 0

    def shift(values, dx, dy, dz):
        moved = pltpu.roll(values, jnp.remainder(-dx + length, length), 0)
        flat = jnp.remainder(2 * cells - dy * length - dz, cells)
        moved = pltpu.roll(moved, flat, 1)
        x, y, z = row + dx, mid + dy, last + dz
        keep = (x >= 0) & (x < length) & (y >= 0) & (y < length) & (z >= 0) & (z < length)
        return jnp.where(keep, moved, 0.0)

    def mirrored(values):
        tiles = []
        for n in range(values.shape[1] // LANES)[::-1]:
            tile = values[:, n * LANES : (n + 1) * LANES]
            tiles.append(jnp.where(flip, pltpu.roll(tile, length, 1), pltpu.roll(tile, LANES - length, 1)))
        return jnp.concatenate(tiles, axis=1)

    def product(values, n):
        count = values.shape[0]
        high, low = split_field(values)
        both = dot(jnp.concatenate([high, low], axis=0), plane_high[n])
        return both[:count] + both[count:] + dot(high, plane_low[n])

    def along_x(values):
        high, low = split_field(values)
        return dot(sine, jnp.concatenate([high, low, high], axis=0))

    def whole(box, b):
        for part in range(regions):
            field[b, part * depth : (part + 1) * depth, :] = box(part).astype(F32)
        return field[b]

    moves = []
    for b in batches:
        r = jnp.int32(0)
        for part in range(regions):
            r = jnp.where(region == part, row_of[b * regions + part], r)
        j = me * local_count + pairs[0, me, r]
        i = lax.div(pairs[2, me, r], cap) * local_count + pairs[1, me, r]
        moves.append([offsets[a, j] - offsets[a, i] for a in range(3)])

    grp_wait(*j_args)
    for b in batches:
        shifted[b] = shift(whole(lambda part: box_j[part, b], b), *moves[b])

    for b in batches:
        away = sum(order[n] > 0 for n in spans[b])
        bytes_of(recv_a[b].at[pl.ds(0, away)], sem_ra.at[b]).wait()
        for n in spans[b]:
            for c in range(cap):
                slots_a[b][n * cap + c] = recv_a[b][n - spans[b][0], c]
        for part in range(regions):
            place = jnp.minimum(place_of[b * regions + part], needed[b] * cap - 1)
            stage_i[b, part] = slots_a[b][place]
        grp_send(*i_args[b])
        box_i[b, region] = stage_i[b, region]
        if b + 1 < share:
            for n in range(needed[b] * cap):
                slots_a[b + 1][n] = slots_a[b][n]

    middle = cells // 2
    for b in batches:
        grp_wait(*i_args[b])
        second[b] = whole(lambda part: box_i[b, part], b)
        charge = second[b] * shifted[b]
        left, right = charge[:, :middle], mirrored(charge[:, middle:])
        field[b, :, :middle] = product(left + right, 0)
        field[b, :, middle:] = product(left - right, 1)
        field[b] = along_x(along_x(field[b]) * green)
        even = product(field[b, :, :middle], 2)
        odd = product(field[b, :, middle:], 3)
        field[b, :, :middle] = even + odd
        field[b, :, middle:] = mirrored(even - odd)
        code, top = encode(field[b] * shifted[b])
        for part in range(regions):
            term_i[b, part] = code[part * depth : (part + 1) * depth, :]
            top_i[b, part] = top
        grp_send(*t_args[b])
        grp_send(*v_args[b])
        rows_i[b][region] = term_i[b, region]
        top_rows[b][region] = top_i[b, region]

    for b in batches:
        term = shift(field[b] * second[b], *[-d for d in moves[b]])
        for part in range(regions):
            term_j[b, part] = term[part * depth : (part + 1) * depth, :]
        rows_j[b, region] = term_j[b, region]

    def term_copies(b, n):
        return (
            orb_copy(n, send_top.at[n], recv_top.at[n], sem_sw.at[0], sem_rw.at[b]),
            orb_copy(n, send_d.at[n], recv_d.at[n], sem_sd.at[0], sem_rd.at[n]),
        )

    sends = []
    for b in batches:
        grp_wait(*t_args[b])
        grp_wait(*v_args[b])
        for part in range(regions):
            for later in range(b, share):
                every_i[later][b * regions + part] = rows_i[b][part]
                every_top[later][b * regions + part] = top_rows[b][part]
        leaving = range(closed[b - 1] if b else 0, closed[b])
        leaving = sorted(leaving, key=lambda n: -order[n])
        for n in leaving:
            for c in range(cap):
                q, _ = find(pairs, me, other(n) * cap + c, lambda r: ranks[r], rows)
                q = jnp.minimum(q, (b + 1) * regions - 1)
                send_d[n, c] = every_i[b][q]
                send_top[n, c : c + 1] = every_top[b][q]
        for n in leaving:
            if order[n]:
                for copy in term_copies(b, n):
                    copy.start()
        sends.append([n for n in leaving if order[n]])
        if b == 0:
            for args in u_args:
                grp_send(*args)

    def arrived(n, codes, tops):
        for c in range(cap):
            landed[n, c] = decode(codes[n, c], tops[n, c : c + 1])

    for n in range(groups):
        if not order[n]:
            arrived(n, send_d, send_top)
    for args in u_args:
        grp_wait(*args)
    for r in range(rows):
        home[r] = rows_j[lax.div(ranks[r], regions), lax.rem(ranks[r], regions)]
    for b in batches:
        bytes_of(recv_top.at[pl.ds(0, len(sends[b]))], sem_rw.at[b]).wait()
        for n in sends[b]:
            bytes_of(recv_d.at[n], sem_rd.at[n]).wait()
            arrived(n, recv_d, recv_top)
    begun.append(bytes_of(send_top.at[pl.ds(0, groups - 1)], sem_sw.at[0]))
    begun.append(bytes_of(send_d.at[pl.ds(0, groups - 1)], sem_sd.at[0]))
    for copy in begun:
        copy.wait()


def exchange_terms(pairs, offsets, orbitals, groups, regions):
    _, depth, cells = orbitals.shape
    rows = pairs.shape[2]
    share = rows // regions
    cap = 2 * rows // groups
    length = depth * regions
    vmem = pl.BlockSpec(memory_space=pltpu.VMEM)
    operands = (pairs, offsets, orbitals, jnp.asarray(fixed_tables(length)))
    spaces = [pltpu.SMEM, pltpu.SMEM, pltpu.VMEM, pltpu.VMEM]
    by_slot = (groups, cap, depth, cells)
    by_batch = (share, regions, depth, cells)
    by_region = (regions, depth, cells)
    dma = pltpu.SemaphoreType.DMA
    one, each, orb_sem = dma((1,)), dma((share,)), dma((groups,))
    _, needed, _ = slot_order(groups, cap, regions, rows)
    parts = [last - first for first, last in zip([0] + needed[:-1], needed)]
    box = (length, cells)
    table = (4, cells // 2, cells // 2)
    i16 = jnp.int16
    return pl.pallas_call(
        exchange_kernel,
        out_shape=(
            jax.ShapeDtypeStruct(by_slot, F32), jax.ShapeDtypeStruct((rows, depth, cells), F32)),
        in_specs=[pl.BlockSpec(memory_space=pltpu.HBM)] * len(operands),
        out_specs=(vmem, vmem),
        scratch_shapes=[
            *[space(x.shape, x.dtype) for space, x in zip(spaces, operands)],
            dma((len(operands),)),
            pltpu.VMEM(by_slot, BF16),
            [pltpu.VMEM((count, cap, depth, cells), BF16) for count in parts],
            [pltpu.VMEM((count * cap, depth, cells), BF16) for count in needed],
            pltpu.VMEM(by_batch, BF16),
            pltpu.VMEM((regions, share, depth, cells), BF16),
            pltpu.VMEM(by_batch, BF16),
            pltpu.VMEM((regions, share, depth, cells), BF16),
            pltpu.VMEM((share, *box), F32), pltpu.VMEM((share, *box), F32),
            pltpu.VMEM((share, *box), F32),
            pltpu.VMEM(table, BF16), pltpu.VMEM(table, BF16),
            pltpu.VMEM(by_batch, i16), pltpu.VMEM(by_batch, F32),
            [pltpu.VMEM(by_region, i16) for _ in range(share)],
            [pltpu.VMEM(((b + 1) * regions, depth, cells), i16) for b in range(share)],
            pltpu.VMEM(by_batch, F32),
            pltpu.VMEM((share, regions, 1, LANES), F32),
            [pltpu.VMEM((regions, 1, LANES), F32) for _ in range(share)],
            [pltpu.VMEM(((b + 1) * regions, 1, LANES), F32) for b in range(share)],
            pltpu.VMEM(by_slot, i16), pltpu.VMEM(by_slot, i16),
            pltpu.VMEM((groups, cap, LANES), F32), pltpu.VMEM((groups, cap, LANES), F32),
            one, each, each, each, one, one, each, each, each, each, one, orb_sem,
            each, each, one, each,
        ],
        compiler_params=pltpu.CompilerParams(
            collective_id=0, has_side_effects=True, vmem_limit_bytes=32 * 1024 * 1024),
    )(*[pltpu.with_memory_space_constraint(x, pltpu.HBM) for x in operands])


def collect_kernel(pairs_in, landed, home, out, pairs, sem_in):
    groups, cap = landed.shape[:2]
    rows = home.shape[0]
    order, _, _ = slot_order(groups, cap, lax.axis_size("grp"), rows)
    me = lax.axis_index("orb")
    load = pltpu.make_async_copy(pairs_in, pairs, sem_in)
    load.start()
    out[...] = jnp.zeros_like(out)
    load.wait()
    for r in range(rows):
        k = pairs[0, me, r]
        out[k] += home[r]
    for n in range(groups):
        block = partner(me, order[n])
        for c in range(cap):
            k, valid = find(pairs, block, me * cap + c, lambda r: pairs[1, block, r], rows)
            out[k] += jnp.where(valid > 0, landed[n, c], 0.0)


def collect(pairs, landed, home, shape):
    vmem = pl.BlockSpec(memory_space=pltpu.VMEM)
    return pl.pallas_call(
        collect_kernel,
        out_shape=jax.ShapeDtypeStruct(shape, F32),
        in_specs=[pl.BlockSpec(memory_space=pltpu.HBM), vmem, vmem],
        out_specs=vmem,
        scratch_shapes=[pltpu.SMEM(pairs.shape, pairs.dtype), pltpu.SemaphoreType.DMA],
        compiler_params=pltpu.CompilerParams(vmem_limit_bytes=32 * 1024 * 1024),
    )(pltpu.with_memory_space_constraint(pairs, pltpu.HBM), landed, home)


def per_device(orbitals, pair_list, offsets):
    groups = lax.axis_size("orb")
    regions = lax.axis_size("grp")
    pairs = jnp.transpose(pair_list, (2, 0, 1))
    landed, home = exchange_terms(pairs, offsets.T, orbitals, groups, regions)
    return collect(pairs, landed, home, orbitals.shape)


def solution(mesh):
    in_specs = (P("orb", "grp", None), P(), P())
    out_specs = P("orb", "grp", None)
    return jax.shard_map(
        per_device, mesh=mesh, in_specs=in_specs, out_specs=out_specs, check_vma=False
    )
```

```python
import math

import jax
import jax.numpy as jnp
import ml_dtypes
import numpy as np
from jax import lax
from jax.experimental import pallas as pl
from jax.experimental.pallas import tpu as pltpu
from jax.sharding import PartitionSpec as P

MESH = pl.DeviceIdType.MESH
SHIFT = 0.25
LANES = 128
F32 = jnp.float32
BF16 = jnp.bfloat16


def split_table(table):
    wide = np.asarray(table, np.float32)
    high = wide.astype(ml_dtypes.bfloat16)
    low = (wide - high.astype(np.float32)).astype(ml_dtypes.bfloat16)
    return high, low


def fixed_tables(length):
    counts = np.arange(length) + 1.0
    sine = np.sqrt(2.0 / (length + 1.0)) * np.sin(
        math.pi * counts[:, None] * counts[None, :] / (length + 1.0)
    )
    levels = 2.0 - 2.0 * np.cos(math.pi * counts / (length + 1.0))
    green = 1.0 / (
        levels[:, None, None] + levels[None, :, None] + levels[None, None, :] + SHIFT
    )
    half = length // 2
    high, low = split_table(sine)
    lane = np.arange(half * half)
    inner = lane % length
    mirror = inner >= half
    y = (lane // LANES * 2 + mirror) * (LANES // length) + lane % LANES // length
    z = np.where(mirror, length - 1 - inner, inner)
    tables, greens = [], []
    for odd_y in (0, 1):
        for odd_z in (0, 1):
            b, c = 2 * (lane // half) + odd_y, 2 * (lane % half) + odd_z
            table = sine[y[:, None], b] * sine[z[:, None], c]
            sign = np.where(mirror & (odd_z == 1), -1.0, 1.0)
            tables += [*split_table(table * sign[:, None]), *split_table(table.T)]
            greens.append(green[:, b, c])
    small = np.concatenate(greens + [np.zeros((length, LANES))], axis=1).astype(np.float32)
    small[:, length * length : length * length + 3 * length] = np.concatenate(
        [high, high, low], axis=1)
    return np.stack(tables), small


def split_field(field):
    high = field.astype(BF16)
    return high, (field - high.astype(F32)).astype(BF16)


def dot(left, right):
    return jnp.dot(left, right, preferred_element_type=F32)


def grp_order(count):
    return sorted(range(1, count), key=lambda k: -min(k, count - k))


def slot_order(groups, cap, regions, rows):
    far = list(range(groups))[::-1]
    share = rows // regions
    needed = [((b + 1) * regions - 1 + groups * cap - rows) // cap + 1 for b in range(share)]
    closed = [(b + 1) * regions // cap for b in range(share - 1)] + [groups]
    late, early = groups - needed[0], closed[0]
    order = far[:early] + far[early + late :] + far[early : early + late]
    return order, needed, closed


def partner(index, offset):
    value, bit = index, 1
    while bit <= offset:
        if offset & bit:
            value = value + bit - 2 * bit * lax.rem(lax.div(index, bit), 2)
        bit *= 2
    return value


def find(pairs, block, wanted, what, rows):
    value = jnp.int32(0)
    valid = jnp.int32(0)
    for r in range(rows):
        hit = pairs[2, block, r] == wanted
        value = jnp.where(hit, what(r), value)
        valid = jnp.where(hit, jnp.int32(1), valid)
    return value, valid


LEVELS = 32766.0


def encode(values):
    size = jnp.abs(values)
    top = jnp.maximum(jnp.max(jnp.max(size, axis=0, keepdims=True), axis=1, keepdims=True), 1e-36)
    steps = (jnp.sqrt(size * (1.0 / top)) * LEVELS + 0.5).astype(jnp.int32)
    code = jnp.where(values < 0.0, -steps, steps).astype(jnp.int16)
    return code, jnp.broadcast_to(top, (1, LANES))


def decode(code, top):
    steps = code.astype(jnp.int32).astype(F32)
    return steps * jnp.abs(steps) * (top[:, 0:1] * (1.0 / (LEVELS * LEVELS)))


def exchange_kernel(
    pairs_in, offsets_in, orbitals_in, tables_in, small_in,
    landed, home, targets,
    pairs, offsets, orbitals, tables, small, sem_in,
    send_a, recv_a, slots_a, stage_i, stage_j, box_i, box_j, field, shifted, second,
    term_i, term_j, rows_i, every_i, rows_j, top_i, top_rows, every_top,
    send_d, recv_d, send_top, recv_top,
    sem_sa, sem_ra, sem_si, sem_ri, sem_sj, sem_rj, sem_st, sem_rt, sem_su, sem_ru, sem_sd, sem_rd,
    sem_sv, sem_rv, sem_sw, sem_rw,
):
    groups, cap, depth, cells = send_a.shape
    share, regions = box_i.shape[:2]
    rows = regions * share
    length = regions * depth
    local_count = orbitals.shape[0]
    me = lax.axis_index("orb")
    region = lax.axis_index("grp")
    grp_steps = grp_order(regions)
    order, needed, closed = slot_order(groups, cap, regions, rows)
    batches = range(share)
    begun = []

    def grp_peer(k):
        return lax.rem(region + k, regions)

    def other(n):
        return partner(me, order[n])

    loads = [
        pltpu.make_async_copy(source, target, sem_in.at[n])
        for n, (source, target) in enumerate((
            (pairs_in, pairs), (orbitals_in, orbitals), (offsets_in, offsets),
            (tables_in, tables), (small_in, small)))
    ]
    for load in loads:
        load.start()
    barrier = pltpu.get_barrier_semaphore()
    for k in range(1, groups):
        pl.semaphore_signal(
            barrier, inc=1, device_id={"orb": lax.rem(me + k, groups)}, device_id_type=MESH)
    for k in grp_steps:
        pl.semaphore_signal(barrier, inc=1, device_id={"grp": grp_peer(k)}, device_id_type=MESH)
    loads[0].wait()

    asked = []
    for n in range(groups):
        block = other(n)
        for c in range(cap):
            asked.append(find(pairs, block, me * cap + c, lambda r: pairs[1, block, r], rows))
    loads[1].wait()
    for n in range(groups):
        for c in range(cap):
            send_a[n, c] = orbitals[asked[n * cap + c][0]]
    pl.semaphore_wait(barrier, groups + regions - 2)

    def orb_copy(n, source, target, send_sem, recv_sem):
        return pltpu.make_async_remote_copy(
            src_ref=source, dst_ref=target, send_sem=send_sem, recv_sem=recv_sem,
            device_id={"orb": other(n)}, device_id_type=MESH)

    def bytes_of(ref, sem):
        return pltpu.make_async_copy(ref, ref, sem)

    def grp_send(source, target, send_sem, recv_sem):
        for k in grp_steps:
            peer = grp_peer(k)
            pltpu.make_async_remote_copy(
                src_ref=source.at[peer], dst_ref=target.at[region],
                send_sem=send_sem, recv_sem=recv_sem,
                device_id={"grp": peer}, device_id_type=MESH).start()
        begun.append(bytes_of(source.at[pl.ds(0, regions - 1)], send_sem))

    def grp_wait(source, target, send_sem, recv_sem):
        bytes_of(target.at[pl.ds(0, regions - 1)], recv_sem).wait()

    j_args = (stage_j, box_j, sem_sj.at[0], sem_rj.at[0])
    i_args = [(stage_i.at[b], box_i.at[b], sem_si.at[b], sem_ri.at[b]) for b in batches]
    t_args = [(term_i.at[b], rows_i[b], sem_st.at[b], sem_rt.at[b]) for b in batches]
    v_args = [(top_i.at[b], top_rows[b], sem_sv.at[b], sem_rv.at[b]) for b in batches]
    u_args = [(term_j.at[b], rows_j.at[b], sem_su.at[b], sem_ru.at[b]) for b in batches]

    spans = [range(needed[b - 1] if b else 0, needed[b]) for b in batches]

    def box_copy(b, n):
        return orb_copy(n, send_a.at[n], recv_a[b].at[n - spans[b][0]], sem_sa.at[0], sem_ra.at[b])

    for b in batches:
        for n in spans[b]:
            if order[n]:
                box_copy(b, n).start()
    begun.append(bytes_of(send_a.at[pl.ds(0, groups - 1)], sem_sa.at[0]))
    places = []
    for r in range(rows):
        slot = pairs[2, me, r]
        group = lax.div(slot, cap)
        place = jnp.int32(0)
        for n in range(groups):
            place = jnp.where(group == other(n), jnp.int32(n * cap), place)
        places.append(place + lax.rem(slot, cap))
    ranks = []
    for r in range(rows):
        rank = jnp.int32(0)
        for q in range(rows):
            if q != r:
                rank = rank + jnp.where(places[q] < places[r], jnp.int32(1), jnp.int32(0))
        ranks.append(rank)

    def ranked(values, rank):
        value = jnp.int32(0)
        for r in range(rows):
            value = jnp.where(ranks[r] == rank, values[r], value)
        return value

    row_of = [ranked([jnp.int32(r) for r in range(rows)], q) for q in range(rows)]
    place_of = [ranked(places, q) for q in range(rows)]

    for b in batches:
        for part in range(regions):
            stage_j[part, b] = orbitals[pairs[0, me, row_of[b * regions + part]]]
    grp_send(*j_args)
    for b in batches:
        for n in spans[b]:
            if not order[n]:
                for c in range(cap):
                    recv_a[b][n - spans[b][0], c] = send_a[n, c]
    box_j[region] = stage_j[region]

    for n, (local, valid) in enumerate(asked):
        targets[0, n] = local
        targets[1, n] = valid
    for r in range(rows):
        targets[2, r] = pairs[0, me, r]

    for load in loads[2:]:
        load.wait()
    sine = small[:, cells : cells + 3 * length].astype(BF16)
    green = small[:, :cells]

    row = lax.broadcasted_iota(jnp.int32, (length, cells), 0)
    col = lax.broadcasted_iota(jnp.int32, (length, cells), 1)
    mid = col // length
    last = col - mid * length
    lane = lax.broadcasted_iota(jnp.int32, (length, LANES), 1)
    inner = lax.rem(lane, length)
    near = inner < length // 2
    flip_y = LANES - length - lane + 2 * inner
    flip_z = lane + length - 1 - 2 * inner

    def shift(values, dx, dy, dz):
        moved = pltpu.roll(values, jnp.remainder(-dx + length, length), 0)
        flat = jnp.remainder(2 * cells - dy * length - dz, cells)
        moved = pltpu.roll(moved, flat, 1)
        x, y, z = row + dx, mid + dy, last + dz
        keep = (x >= 0) & (x < length) & (y >= 0) & (y < length) & (z >= 0) & (z < length)
        return jnp.where(keep, moved, 0.0)

    def taken(tile, index):
        return jnp.take_along_axis(tile, index, axis=1)

    def joined(tiles):
        return jnp.concatenate(tiles, axis=1)

    def folded(values):
        count = cells // LANES
        tiles = [values[:, n * LANES : (n + 1) * LANES] for n in range(count)]
        far = [taken(tiles[count - 1 - n], flip_y) for n in range(count // 2)]
        quarters = []
        for side in (1.0, -1.0):
            half = [tile + other if side > 0 else tile - other for tile, other in zip(tiles, far)]
            back = [taken(tile, flip_z) for tile in half]
            even = [tile + other for tile, other in zip(half, back)]
            odd = [tile - other for tile, other in zip(half, back)]
            for part in (even, odd):
                quarters.append(joined(
                    [jnp.where(near, part[n], part[n + 1]) for n in range(0, count // 2, 2)]))
        return quarters

    def unfolded(quarters):
        count = cells // LANES
        halves = []
        for even, odd in (quarters[:2], quarters[2:]):
            total, rest = even + odd, even - odd
            tiles = []
            for n in range(count // 4):
                here = slice(n * LANES, (n + 1) * LANES)
                tiles.append(jnp.where(near, total[:, here], taken(rest[:, here], flip_z)))
                tiles.append(jnp.where(near, taken(total[:, here], flip_z), rest[:, here]))
            halves.append(tiles)
        first = [even + odd for even, odd in zip(*halves)]
        return joined(first + [taken(even - odd, flip_y) for even, odd in zip(*halves)][::-1])

    def product(values, n):
        count = values.shape[0]
        high, low = split_field(values)
        both = dot(jnp.concatenate([high, low], axis=0), tables[2 * n])
        return both[:count] + both[count:] + dot(high, tables[2 * n + 1])

    def along_x(values):
        high, low = split_field(values)
        return dot(sine, jnp.concatenate([high, low, high], axis=0))

    def whole(box, b):
        for part in range(regions):
            field[b, part * depth : (part + 1) * depth, :] = box(part).astype(F32)
        return field[b]

    moves = []
    for b in batches:
        r = jnp.int32(0)
        for part in range(regions):
            r = jnp.where(region == part, row_of[b * regions + part], r)
        j = me * local_count + pairs[0, me, r]
        i = lax.div(pairs[2, me, r], cap) * local_count + pairs[1, me, r]
        moves.append([offsets[a, j] - offsets[a, i] for a in range(3)])

    grp_wait(*j_args)
    for b in batches:
        shifted[b] = shift(whole(lambda part: box_j[part, b], b), *moves[b])

    for b in batches:
        away = sum(order[n] > 0 for n in spans[b])
        bytes_of(recv_a[b].at[pl.ds(0, away)], sem_ra.at[b]).wait()
        for n in spans[b]:
            for c in range(cap):
                slots_a[b][n * cap + c] = recv_a[b][n - spans[b][0], c]
        for part in range(regions):
            place = jnp.minimum(place_of[b * regions + part], needed[b] * cap - 1)
            stage_i[b, part] = slots_a[b][place]
        grp_send(*i_args[b])
        box_i[b, region] = stage_i[b, region]
        if b + 1 < share:
            for n in range(needed[b] * cap):
                slots_a[b + 1][n] = slots_a[b][n]

    quarter = cells // 4
    for b in batches:
        grp_wait(*i_args[b])
        second[b] = whole(lambda part: box_i[b, part], b)
        charge = second[b] * shifted[b]
        spectrum = joined([product(part, 2 * q) for q, part in enumerate(folded(charge))])
        spectrum = along_x(along_x(spectrum) * green)
        field[b] = unfolded([
            product(spectrum[:, q * quarter : (q + 1) * quarter], 2 * q + 1) for q in range(4)])
        code, top = encode(field[b] * shifted[b])
        for part in range(regions):
            term_i[b, part] = code[part * depth : (part + 1) * depth, :]
            top_i[b, part] = top
        grp_send(*t_args[b])
        grp_send(*v_args[b])
        rows_i[b][region] = term_i[b, region]
        top_rows[b][region] = top_i[b, region]

    for b in batches:
        term = shift(field[b] * second[b], *[-d for d in moves[b]])
        for part in range(regions):
            term_j[b, part] = term[part * depth : (part + 1) * depth, :]
        rows_j[b, region] = term_j[b, region]

    def term_copies(b, n):
        return (
            orb_copy(n, send_top.at[n], recv_top.at[n], sem_sw.at[0], sem_rw.at[b]),
            orb_copy(n, send_d.at[n], recv_d.at[n], sem_sd.at[0], sem_rd.at[n]),
        )

    sends = []
    for b in batches:
        grp_wait(*t_args[b])
        grp_wait(*v_args[b])
        for part in range(regions):
            for later in range(b, share):
                every_i[later][b * regions + part] = rows_i[b][part]
                every_top[later][b * regions + part] = top_rows[b][part]
        leaving = range(closed[b - 1] if b else 0, closed[b])
        leaving = sorted(leaving, key=lambda n: -order[n])
        for n in leaving:
            for c in range(cap):
                q, _ = find(pairs, me, other(n) * cap + c, lambda r: ranks[r], rows)
                q = jnp.minimum(q, (b + 1) * regions - 1)
                send_d[n, c] = every_i[b][q]
                send_top[n, c : c + 1] = every_top[b][q]
        for n in leaving:
            if order[n]:
                for copy in term_copies(b, n):
                    copy.start()
        sends.append([n for n in leaving if order[n]])
        if b == 0:
            for args in u_args:
                grp_send(*args)

    def arrived(n, codes, tops):
        for c in range(cap):
            landed[n, c] = decode(codes[n, c], tops[n, c : c + 1])

    for n in range(groups):
        if not order[n]:
            arrived(n, send_d, send_top)
    for args in u_args:
        grp_wait(*args)
    for r in range(rows):
        home[r] = rows_j[lax.div(ranks[r], regions), lax.rem(ranks[r], regions)]
    for b in batches:
        bytes_of(recv_top.at[pl.ds(0, len(sends[b]))], sem_rw.at[b]).wait()
        for n in sends[b]:
            bytes_of(recv_d.at[n], sem_rd.at[n]).wait()
            arrived(n, recv_d, recv_top)
    begun.append(bytes_of(send_top.at[pl.ds(0, groups - 1)], sem_sw.at[0]))
    begun.append(bytes_of(send_d.at[pl.ds(0, groups - 1)], sem_sd.at[0]))
    for copy in begun:
        copy.wait()


def exchange_terms(pairs, offsets, orbitals, groups, regions):
    _, depth, cells = orbitals.shape
    rows = pairs.shape[2]
    share = rows // regions
    cap = 2 * rows // groups
    length = depth * regions
    vmem = pl.BlockSpec(memory_space=pltpu.VMEM)
    operands = (pairs, offsets, orbitals, *[jnp.asarray(t) for t in fixed_tables(length)])
    spaces = [pltpu.SMEM, pltpu.SMEM] + [pltpu.VMEM] * 3
    by_slot = (groups, cap, depth, cells)
    by_batch = (share, regions, depth, cells)
    by_region = (regions, depth, cells)
    dma = pltpu.SemaphoreType.DMA
    one, each, orb_sem = dma((1,)), dma((share,)), dma((groups,))
    _, needed, _ = slot_order(groups, cap, regions, rows)
    parts = [last - first for first, last in zip([0] + needed[:-1], needed)]
    box = (length, cells)
    i16 = jnp.int16
    return pl.pallas_call(
        exchange_kernel,
        out_shape=(
            jax.ShapeDtypeStruct(by_slot, F32), jax.ShapeDtypeStruct((rows, depth, cells), F32),
            pltpu.SMEM((3, groups * cap), jnp.int32)),
        in_specs=[pl.BlockSpec(memory_space=pltpu.HBM)] * len(operands),
        out_specs=(vmem, vmem, pl.BlockSpec(memory_space=pltpu.SMEM)),
        scratch_shapes=[
            *[space(x.shape, x.dtype) for space, x in zip(spaces, operands)],
            dma((len(operands),)),
            pltpu.VMEM(by_slot, BF16),
            [pltpu.VMEM((count, cap, depth, cells), BF16) for count in parts],
            [pltpu.VMEM((count * cap, depth, cells), BF16) for count in needed],
            pltpu.VMEM(by_batch, BF16),
            pltpu.VMEM((regions, share, depth, cells), BF16),
            pltpu.VMEM(by_batch, BF16),
            pltpu.VMEM((regions, share, depth, cells), BF16),
            pltpu.VMEM((share, *box), F32), pltpu.VMEM((share, *box), F32),
            pltpu.VMEM((share, *box), F32),
            pltpu.VMEM(by_batch, i16), pltpu.VMEM(by_batch, F32),
            [pltpu.VMEM(by_region, i16) for _ in range(share)],
            [pltpu.VMEM(((b + 1) * regions, depth, cells), i16) for b in range(share)],
            pltpu.VMEM(by_batch, F32),
            pltpu.VMEM((share, regions, 1, LANES), F32),
            [pltpu.VMEM((regions, 1, LANES), F32) for _ in range(share)],
            [pltpu.VMEM(((b + 1) * regions, 1, LANES), F32) for b in range(share)],
            pltpu.VMEM(by_slot, i16), pltpu.VMEM(by_slot, i16),
            pltpu.VMEM((groups, cap, LANES), F32), pltpu.VMEM((groups, cap, LANES), F32),
            one, each, each, each, one, one, each, each, each, each, one, orb_sem,
            each, each, one, each,
        ],
        compiler_params=pltpu.CompilerParams(
            collective_id=0, has_side_effects=True, vmem_limit_bytes=32 * 1024 * 1024),
    )(*[pltpu.with_memory_space_constraint(x, pltpu.HBM) for x in operands])


def collect_kernel(landed, home, targets, out):
    groups, cap = landed.shape[:2]
    out[...] = jnp.zeros_like(out)
    for r in range(home.shape[0]):
        out[targets[2, r]] += home[r]
    for n in range(groups):
        for c in range(cap):
            slot = n * cap + c
            out[targets[0, slot]] += jnp.where(targets[1, slot] > 0, landed[n, c], 0.0)


def collect(landed, home, targets, shape):
    vmem = pl.BlockSpec(memory_space=pltpu.VMEM)
    return pl.pallas_call(
        collect_kernel,
        out_shape=jax.ShapeDtypeStruct(shape, F32),
        in_specs=[vmem, vmem, pl.BlockSpec(memory_space=pltpu.SMEM)],
        out_specs=vmem,
        compiler_params=pltpu.CompilerParams(vmem_limit_bytes=32 * 1024 * 1024),
    )(landed, home, pltpu.with_memory_space_constraint(targets, pltpu.SMEM))


def per_device(orbitals, pair_list, offsets):
    groups = lax.axis_size("orb")
    regions = lax.axis_size("grp")
    pairs = jnp.transpose(pair_list, (2, 0, 1))
    landed, home, targets = exchange_terms(pairs, offsets.T, orbitals, groups, regions)
    return collect(landed, home, targets, orbitals.shape)


def solution(mesh):
    in_specs = (P("orb", "grp", None), P(), P())
    out_specs = P("orb", "grp", None)
    return jax.shard_map(
        per_device, mesh=mesh, in_specs=in_specs, out_specs=out_specs, check_vma=False
    )
```

```python
import math

import jax
import jax.numpy as jnp
import ml_dtypes
import numpy as np
from jax import lax
from jax.experimental import pallas as pl
from jax.experimental.pallas import tpu as pltpu
from jax.sharding import PartitionSpec as P

MESH = pl.DeviceIdType.MESH
SHIFT = 0.25
LANES = 128
F32 = jnp.float32
BF16 = jnp.bfloat16


def split_table(table):
    wide = np.asarray(table, np.float32)
    high = wide.astype(ml_dtypes.bfloat16)
    low = (wide - high.astype(np.float32)).astype(ml_dtypes.bfloat16)
    return high, low


def fixed_tables(length):
    counts = np.arange(length) + 1.0
    sine = np.sqrt(2.0 / (length + 1.0)) * np.sin(
        math.pi * counts[:, None] * counts[None, :] / (length + 1.0)
    )
    levels = 2.0 - 2.0 * np.cos(math.pi * counts / (length + 1.0))
    green = 1.0 / (
        levels[:, None, None] + levels[None, :, None] + levels[None, None, :] + SHIFT
    )
    half = length // 2
    high, low = split_table(sine)
    lane = np.arange(half * half)
    inner = lane % length
    mirror = inner >= half
    y = (lane // LANES * 2 + mirror) * (LANES // length) + lane % LANES // length
    z = np.where(mirror, length - 1 - inner, inner)
    tables, greens = [], []
    for odd_y in (0, 1):
        for odd_z in (0, 1):
            b, c = 2 * (lane // half) + odd_y, 2 * (lane % half) + odd_z
            table = sine[y[:, None], b] * sine[z[:, None], c]
            sign = np.where(mirror & (odd_z == 1), -1.0, 1.0)
            tables += [*split_table(table * sign[:, None]), *split_table(table.T)]
            greens.append(green[:, b, c])
    small = np.concatenate(greens + [np.zeros((length, LANES))], axis=1).astype(np.float32)
    small[:, length * length : length * length + 3 * length] = np.concatenate(
        [high, high, low], axis=1)
    return np.stack(tables), small


def split_field(field):
    high = field.astype(BF16)
    return high, (field - high.astype(F32)).astype(BF16)


def dot(left, right):
    return jnp.dot(left, right, preferred_element_type=F32)


def slot_order(groups, cap, regions, rows):
    far = list(range(groups))[::-1]
    share = rows // regions
    needed = [((b + 1) * regions - 1 + groups * cap - rows) // cap + 1 for b in range(share)]
    closed = [(b + 1) * regions // cap for b in range(share - 1)] + [groups]
    late, early = groups - needed[0], closed[0]
    order = far[:early] + far[early + late :] + far[early : early + late]
    return order, needed, closed


def partner(index, offset):
    value, bit = index, 1
    while bit <= offset:
        if offset & bit:
            value = value + bit - 2 * bit * lax.rem(lax.div(index, bit), 2)
        bit *= 2
    return value


def find(pairs, block, wanted, what, rows):
    value = jnp.int32(0)
    valid = jnp.int32(0)
    for r in range(rows):
        hit = pairs[2, block, r] == wanted
        value = jnp.where(hit, what(r), value)
        valid = jnp.where(hit, jnp.int32(1), valid)
    return value, valid


LEVELS = 32766.0


def encode(values):
    size = jnp.abs(values)
    top = jnp.maximum(jnp.max(jnp.max(size, axis=0, keepdims=True), axis=1, keepdims=True), 1e-36)
    steps = (jnp.sqrt(size * (1.0 / top)) * LEVELS + 0.5).astype(jnp.int32)
    code = jnp.where(values < 0.0, -steps, steps).astype(jnp.int16)
    return code, jnp.broadcast_to(top, (1, LANES))


def decode(code, top):
    steps = code.astype(jnp.int32).astype(F32)
    return steps * jnp.abs(steps) * (top[:, 0:1] * (1.0 / (LEVELS * LEVELS)))


def exchange_kernel(
    pairs_in, offsets_in, orbitals_in, tables_in, small_in,
    landed, home, targets,
    pairs, offsets, orbitals, tables, small, sem_in,
    send_a, recv_a, slots_a, stage_i, stage_j, box_i, box_j, field, shifted, second,
    term_i, term_j, rows_i, every_i, rows_j, top_i, top_rows, every_top,
    send_d, recv_d, send_top, recv_top,
    sem_sa, sem_ra, sem_si, sem_ri, sem_sj, sem_rj, sem_st, sem_rt, sem_su, sem_ru, sem_sd, sem_rd,
    sem_sv, sem_rv, sem_sw, sem_rw,
):
    groups, cap, depth, cells = send_a.shape
    share, regions = box_i.shape[:2]
    rows = regions * share
    length = regions * depth
    local_count = orbitals.shape[0]
    me = lax.axis_index("orb")
    region = lax.axis_index("grp")
    grp_steps = range(regions)[:0:-1]
    order, needed, closed = slot_order(groups, cap, regions, rows)
    batches = range(share)
    begun = []

    def grp_peer(k):
        return partner(region, k)

    def other(n):
        return partner(me, order[n])

    loads = [
        pltpu.make_async_copy(source, target, sem_in.at[n])
        for n, (source, target) in enumerate((
            (pairs_in, pairs), (orbitals_in, orbitals), (offsets_in, offsets),
            (tables_in, tables), (small_in, small)))
    ]
    for load in loads:
        load.start()
    barrier = pltpu.get_barrier_semaphore()
    for k in range(1, groups):
        pl.semaphore_signal(
            barrier, inc=1, device_id={"orb": lax.rem(me + k, groups)}, device_id_type=MESH)
    for k in grp_steps:
        pl.semaphore_signal(barrier, inc=1, device_id={"grp": grp_peer(k)}, device_id_type=MESH)
    loads[0].wait()

    asked = []
    for n in range(groups):
        block = other(n)
        for c in range(cap):
            asked.append(find(pairs, block, me * cap + c, lambda r: pairs[1, block, r], rows))
    loads[1].wait()
    for n in range(groups):
        for c in range(cap):
            send_a[n, c] = orbitals[asked[n * cap + c][0]]
    pl.semaphore_wait(barrier, groups + regions - 2)

    def orb_copy(peer, source, target, send_sem, recv_sem):
        return pltpu.make_async_remote_copy(
            src_ref=source, dst_ref=target, send_sem=send_sem, recv_sem=recv_sem,
            device_id={"orb": peer}, device_id_type=MESH)

    def pair_places(n):
        chip = order[n] // 2
        if chip == 0:
            return [(n, other(n))]
        core = lax.rem(me, 2)
        base = 2 * partner(lax.div(me, 2), chip)
        return [(n + 1 - core, base), (n + core, base + 1)]

    def bytes_of(ref, sem):
        return pltpu.make_async_copy(ref, ref, sem)

    def grp_send(source, target, send_sem, recv_sem):
        for k in grp_steps:
            peer = grp_peer(k)
            pltpu.make_async_remote_copy(
                src_ref=source.at[peer], dst_ref=target.at[region],
                send_sem=send_sem, recv_sem=recv_sem,
                device_id={"grp": peer}, device_id_type=MESH).start()
        begun.append(bytes_of(source.at[pl.ds(0, regions - 1)], send_sem))

    def grp_wait(source, target, send_sem, recv_sem):
        bytes_of(target.at[pl.ds(0, regions - 1)], recv_sem).wait()

    j_args = (stage_j, box_j, sem_sj.at[0], sem_rj.at[0])
    i_args = [(stage_i.at[b], box_i.at[b], sem_si.at[b], sem_ri.at[b]) for b in batches]
    t_args = [(term_i.at[b], rows_i[b], sem_st.at[b], sem_rt.at[b]) for b in batches]
    v_args = [(top_i.at[b], top_rows[b], sem_sv.at[b], sem_rv.at[b]) for b in batches]
    u_args = [(term_j.at[b], rows_j.at[b], sem_su.at[b], sem_ru.at[b]) for b in batches]

    spans = [range(needed[b - 1] if b else 0, needed[b]) for b in batches]

    for b in batches:
        for pair in spans[b][::2]:
            for n, peer in pair_places(pair):
                orb_copy(
                    peer, send_a.at[n], recv_a[b].at[n - spans[b][0]], sem_sa.at[0], sem_ra.at[b],
                ).start()
    begun.append(bytes_of(send_a.at[pl.ds(0, groups - 1)], sem_sa.at[0]))
    places = []
    for r in range(rows):
        slot = pairs[2, me, r]
        group = lax.div(slot, cap)
        place = jnp.int32(0)
        for n in range(groups):
            place = jnp.where(group == other(n), jnp.int32(n * cap), place)
        places.append(place + lax.rem(slot, cap))
    ranks = []
    for r in range(rows):
        rank = jnp.int32(0)
        for q in range(rows):
            if q != r:
                rank = rank + jnp.where(places[q] < places[r], jnp.int32(1), jnp.int32(0))
        ranks.append(rank)

    def ranked(values, rank):
        value = jnp.int32(0)
        for r in range(rows):
            value = jnp.where(ranks[r] == rank, values[r], value)
        return value

    row_of = [ranked([jnp.int32(r) for r in range(rows)], q) for q in range(rows)]
    place_of = [ranked(places, q) for q in range(rows)]
    rank_of = [
        find(pairs, me, other(n) * cap + c, lambda r: ranks[r], rows)[0]
        for n in range(groups) for c in range(cap)]

    for b in batches:
        for part in range(regions):
            stage_j[part, b] = orbitals[pairs[0, me, row_of[b * regions + part]]]
    grp_send(*j_args)
    for b in batches:
        for n in spans[b]:
            if not order[n]:
                for c in range(cap):
                    recv_a[b][n - spans[b][0], c] = send_a[n, c]
    box_j[region] = stage_j[region]

    for n, (local, valid) in enumerate(asked):
        targets[0, n] = local
        targets[1, n] = valid
    for r in range(rows):
        targets[2, r] = pairs[0, me, r]

    for load in loads[2:]:
        load.wait()
    sine = small[:, cells : cells + 3 * length].astype(BF16)
    green = small[:, :cells]

    row = lax.broadcasted_iota(jnp.int32, (length, cells), 0)
    col = lax.broadcasted_iota(jnp.int32, (length, cells), 1)
    mid = col // length
    last = col - mid * length
    lane = lax.broadcasted_iota(jnp.int32, (length, LANES), 1)
    inner = lax.rem(lane, length)
    near = inner < length // 2
    flip_y = LANES - length - lane + 2 * inner
    flip_z = lane + length - 1 - 2 * inner

    def shift(values, dx, dy, dz):
        moved = pltpu.roll(values, jnp.remainder(-dx + length, length), 0)
        flat = jnp.remainder(2 * cells - dy * length - dz, cells)
        moved = pltpu.roll(moved, flat, 1)
        x, y, z = row + dx, mid + dy, last + dz
        keep = (x >= 0) & (x < length) & (y >= 0) & (y < length) & (z >= 0) & (z < length)
        return jnp.where(keep, moved, 0.0)

    def taken(tile, index):
        return jnp.take_along_axis(tile, index, axis=1)

    def joined(tiles):
        return jnp.concatenate(tiles, axis=1)

    def folded(values):
        count = cells // LANES
        tiles = [values[:, n * LANES : (n + 1) * LANES] for n in range(count)]
        far = [taken(tiles[count - 1 - n], flip_y) for n in range(count // 2)]
        quarters = []
        for side in (1.0, -1.0):
            half = [tile + other if side > 0 else tile - other for tile, other in zip(tiles, far)]
            back = [taken(tile, flip_z) for tile in half]
            even = [tile + other for tile, other in zip(half, back)]
            odd = [tile - other for tile, other in zip(half, back)]
            for part in (even, odd):
                quarters.append(joined(
                    [jnp.where(near, part[n], part[n + 1]) for n in range(0, count // 2, 2)]))
        return quarters

    def unfolded(quarters):
        count = cells // LANES
        halves = []
        for even, odd in (quarters[:2], quarters[2:]):
            total, rest = even + odd, even - odd
            tiles = []
            for n in range(count // 4):
                here = slice(n * LANES, (n + 1) * LANES)
                tiles.append(jnp.where(near, total[:, here], taken(rest[:, here], flip_z)))
                tiles.append(jnp.where(near, taken(total[:, here], flip_z), rest[:, here]))
            halves.append(tiles)
        first = [even + odd for even, odd in zip(*halves)]
        return joined(first + [taken(even - odd, flip_y) for even, odd in zip(*halves)][::-1])

    def product(values, n):
        count = values.shape[0]
        high, low = split_field(values)
        both = dot(jnp.concatenate([high, low], axis=0), tables[2 * n])
        return both[:count] + both[count:] + dot(high, tables[2 * n + 1])

    def along_x(values):
        high, low = split_field(values)
        return dot(sine, jnp.concatenate([high, low, high], axis=0))

    def whole(box, b):
        for part in range(regions):
            field[b, part * depth : (part + 1) * depth, :] = box(part).astype(F32)
        return field[b]

    moves = []
    for b in batches:
        r = jnp.int32(0)
        for part in range(regions):
            r = jnp.where(region == part, row_of[b * regions + part], r)
        j = me * local_count + pairs[0, me, r]
        i = lax.div(pairs[2, me, r], cap) * local_count + pairs[1, me, r]
        moves.append([offsets[a, j] - offsets[a, i] for a in range(3)])

    grp_wait(*j_args)
    for b in batches:
        shifted[b] = shift(whole(lambda part: box_j[part, b], b), *moves[b])

    for b in batches:
        away = sum(order[n] > 0 for n in spans[b])
        bytes_of(recv_a[b].at[pl.ds(0, away)], sem_ra.at[b]).wait()
        for n in spans[b]:
            for c in range(cap):
                slots_a[b][n * cap + c] = recv_a[b][n - spans[b][0], c]
        for part in range(regions):
            place = jnp.minimum(place_of[b * regions + part], needed[b] * cap - 1)
            stage_i[b, part] = slots_a[b][place]
        grp_send(*i_args[b])
        box_i[b, region] = stage_i[b, region]
        if b + 1 < share:
            for n in range(needed[b] * cap):
                slots_a[b + 1][n] = slots_a[b][n]

    quarter = cells // 4
    for b in batches:
        grp_wait(*i_args[b])
        second[b] = whole(lambda part: box_i[b, part], b)
        charge = second[b] * shifted[b]
        spectrum = joined([product(part, 2 * q) for q, part in enumerate(folded(charge))])
        spectrum = along_x(along_x(spectrum) * green)
        field[b] = unfolded([
            product(spectrum[:, q * quarter : (q + 1) * quarter], 2 * q + 1) for q in range(4)])
        code, top = encode(field[b] * shifted[b])
        for part in range(regions):
            term_i[b, part] = code[part * depth : (part + 1) * depth, :]
            top_i[b, part] = top
        grp_send(*t_args[b])
        grp_send(*v_args[b])
        rows_i[b][region] = term_i[b, region]
        top_rows[b][region] = top_i[b, region]

    for b in batches:
        term = shift(field[b] * second[b], *[-d for d in moves[b]])
        for part in range(regions):
            term_j[b, part] = term[part * depth : (part + 1) * depth, :]
        rows_j[b, region] = term_j[b, region]

    sends = []
    for b in batches:
        grp_wait(*t_args[b])
        grp_wait(*v_args[b])
        for part in range(regions):
            for later in range(b, share):
                every_i[later][b * regions + part] = rows_i[b][part]
                every_top[later][b * regions + part] = top_rows[b][part]
        leaving = range(closed[b - 1] if b else 0, closed[b])
        for n in leaving:
            for c in range(cap):
                q = jnp.minimum(rank_of[n * cap + c], (b + 1) * regions - 1)
                send_d[n, c] = every_i[b][q]
                send_top[n, c : c + 1] = every_top[b][q]
        pairs_leaving = sorted(leaving[::2], key=lambda n: -order[n])
        for pair in pairs_leaving:
            for n, peer in pair_places(pair):
                orb_copy(
                    peer, send_top.at[n], recv_top.at[n], sem_sw.at[0], sem_rw.at[b]).start()
                orb_copy(
                    peer, send_d.at[n], recv_d.at[n], sem_sd.at[0], sem_rd.at[pair // 2]).start()
        sends.append(pairs_leaving)
        if b == 0:
            for args in u_args:
                grp_send(*args)

    def arrived(n, codes, tops):
        for c in range(cap):
            landed[n, c] = decode(codes[n, c], tops[n, c : c + 1])

    for n in range(groups):
        if not order[n]:
            arrived(n, send_d, send_top)
    for args in u_args:
        grp_wait(*args)
    for r in range(rows):
        home[r] = rows_j[lax.div(ranks[r], regions), lax.rem(ranks[r], regions)]
    for b in batches:
        away = [[n for n in (pair, pair + 1) if order[n]] for pair in sends[b]]
        bytes_of(recv_top.at[pl.ds(0, sum(map(len, away)))], sem_rw.at[b]).wait()
        for pair, both in zip(sends[b], away):
            bytes_of(recv_d.at[pl.ds(pair, len(both))], sem_rd.at[pair // 2]).wait()
            for n in both:
                arrived(n, recv_d, recv_top)
    begun.append(bytes_of(send_top.at[pl.ds(0, groups - 1)], sem_sw.at[0]))
    begun.append(bytes_of(send_d.at[pl.ds(0, groups - 1)], sem_sd.at[0]))
    for copy in begun:
        copy.wait()


def exchange_terms(pairs, offsets, orbitals, groups, regions):
    _, depth, cells = orbitals.shape
    rows = pairs.shape[2]
    share = rows // regions
    cap = 2 * rows // groups
    length = depth * regions
    vmem = pl.BlockSpec(memory_space=pltpu.VMEM)
    operands = (pairs, offsets, orbitals, *[jnp.asarray(t) for t in fixed_tables(length)])
    spaces = [pltpu.SMEM, pltpu.SMEM] + [pltpu.VMEM] * 3
    by_slot = (groups, cap, depth, cells)
    by_batch = (share, regions, depth, cells)
    by_region = (regions, depth, cells)
    dma = pltpu.SemaphoreType.DMA
    one, each, orb_sem = dma((1,)), dma((share,)), dma((groups // 2,))
    _, needed, _ = slot_order(groups, cap, regions, rows)
    parts = [last - first for first, last in zip([0] + needed[:-1], needed)]
    box = (length, cells)
    i16 = jnp.int16
    return pl.pallas_call(
        exchange_kernel,
        out_shape=(
            jax.ShapeDtypeStruct(by_slot, F32), jax.ShapeDtypeStruct((rows, depth, cells), F32),
            pltpu.SMEM((3, groups * cap), jnp.int32)),
        in_specs=[pl.BlockSpec(memory_space=pltpu.HBM)] * len(operands),
        out_specs=(vmem, vmem, pl.BlockSpec(memory_space=pltpu.SMEM)),
        scratch_shapes=[
            *[space(x.shape, x.dtype) for space, x in zip(spaces, operands)],
            dma((len(operands),)),
            pltpu.VMEM(by_slot, BF16),
            [pltpu.VMEM((count, cap, depth, cells), BF16) for count in parts],
            [pltpu.VMEM((count * cap, depth, cells), BF16) for count in needed],
            pltpu.VMEM(by_batch, BF16),
            pltpu.VMEM((regions, share, depth, cells), BF16),
            pltpu.VMEM(by_batch, BF16),
            pltpu.VMEM((regions, share, depth, cells), BF16),
            pltpu.VMEM((share, *box), F32), pltpu.VMEM((share, *box), F32),
            pltpu.VMEM((share, *box), F32),
            pltpu.VMEM(by_batch, i16), pltpu.VMEM(by_batch, F32),
            [pltpu.VMEM(by_region, i16) for _ in range(share)],
            [pltpu.VMEM(((b + 1) * regions, depth, cells), i16) for b in range(share)],
            pltpu.VMEM(by_batch, F32),
            pltpu.VMEM((share, regions, 1, LANES), F32),
            [pltpu.VMEM((regions, 1, LANES), F32) for _ in range(share)],
            [pltpu.VMEM(((b + 1) * regions, 1, LANES), F32) for b in range(share)],
            pltpu.VMEM(by_slot, i16), pltpu.VMEM(by_slot, i16),
            pltpu.VMEM((groups, cap, LANES), F32), pltpu.VMEM((groups, cap, LANES), F32),
            one, each, each, each, one, one, each, each, each, each, one, orb_sem,
            each, each, one, each,
        ],
        compiler_params=pltpu.CompilerParams(
            collective_id=0, has_side_effects=True, vmem_limit_bytes=32 * 1024 * 1024),
    )(*[pltpu.with_memory_space_constraint(x, pltpu.HBM) for x in operands])


def collect_kernel(landed, home, targets, out):
    groups, cap = landed.shape[:2]
    out[...] = jnp.zeros_like(out)
    for r in range(home.shape[0]):
        out[targets[2, r]] += home[r]
    for n in range(groups):
        for c in range(cap):
            slot = n * cap + c
            out[targets[0, slot]] += jnp.where(targets[1, slot] > 0, landed[n, c], 0.0)


def collect(landed, home, targets, shape):
    vmem = pl.BlockSpec(memory_space=pltpu.VMEM)
    return pl.pallas_call(
        collect_kernel,
        out_shape=jax.ShapeDtypeStruct(shape, F32),
        in_specs=[vmem, vmem, pl.BlockSpec(memory_space=pltpu.SMEM)],
        out_specs=vmem,
        compiler_params=pltpu.CompilerParams(vmem_limit_bytes=32 * 1024 * 1024),
    )(landed, home, pltpu.with_memory_space_constraint(targets, pltpu.SMEM))


def per_device(orbitals, pair_list, offsets):
    groups = lax.axis_size("orb")
    regions = lax.axis_size("grp")
    pairs = jnp.transpose(pair_list, (2, 0, 1))
    landed, home, targets = exchange_terms(pairs, offsets.T, orbitals, groups, regions)
    return collect(landed, home, targets, orbitals.shape)


def solution(mesh):
    in_specs = (P("orb", "grp", None), P(), P())
    out_specs = P("orb", "grp", None)
    return jax.shard_map(
        per_device, mesh=mesh, in_specs=in_specs, out_specs=out_specs, check_vma=False
    )
```

```python
import math

import jax
import jax.numpy as jnp
import ml_dtypes
import numpy as np
from jax import lax
from jax.experimental import pallas as pl
from jax.experimental.pallas import tpu as pltpu
from jax.sharding import PartitionSpec as P

MESH = pl.DeviceIdType.MESH
SHIFT = 0.25
LANES = 128
F32 = jnp.float32
BF16 = jnp.bfloat16


def split_table(table):
    wide = np.asarray(table, np.float32)
    high = wide.astype(ml_dtypes.bfloat16)
    low = (wide - high.astype(np.float32)).astype(ml_dtypes.bfloat16)
    return high, low


def fixed_tables(length):
    counts = np.arange(length) + 1.0
    sine = np.sqrt(2.0 / (length + 1.0)) * np.sin(
        math.pi * counts[:, None] * counts[None, :] / (length + 1.0)
    )
    levels = 2.0 - 2.0 * np.cos(math.pi * counts / (length + 1.0))
    green = 1.0 / (
        levels[:, None, None] + levels[None, :, None] + levels[None, None, :] + SHIFT
    )
    half = length // 2
    high, low = split_table(sine)
    lane = np.arange(half * half)
    inner = lane % length
    mirror = inner >= half
    y = (lane // LANES * 2 + mirror) * (LANES // length) + lane % LANES // length
    z = np.where(mirror, length - 1 - inner, inner)
    tables, greens = [], []
    for odd_y in (0, 1):
        for odd_z in (0, 1):
            b, c = 2 * (lane // half) + odd_y, 2 * (lane % half) + odd_z
            table = sine[y[:, None], b] * sine[z[:, None], c]
            sign = np.where(mirror & (odd_z == 1), -1.0, 1.0)
            tables += [*split_table(table * sign[:, None]), *split_table(table.T)]
            greens.append(green[:, b, c])
    small = np.concatenate(greens + [np.zeros((length, LANES))], axis=1).astype(np.float32)
    small[:, length * length : length * length + 3 * length] = np.concatenate(
        [high, high, low], axis=1)
    return np.stack(tables), small


def split_field(field):
    high = field.astype(BF16)
    return high, (field - high.astype(F32)).astype(BF16)


def dot(left, right):
    return jnp.dot(left, right, preferred_element_type=F32)


def slot_order(groups, cap, regions, rows):
    far = list(range(groups))[::-1]
    share = rows // regions
    needed = [((b + 1) * regions - 1 + groups * cap - rows) // cap + 1 for b in range(share)]
    closed = [(b + 1) * regions // cap for b in range(share - 1)] + [groups]
    late, early = groups - needed[0], closed[0]
    order = far[:early] + far[early + late :] + far[early : early + late]
    return order, needed, closed


def partner(index, offset):
    value, bit = index, 1
    while bit <= offset:
        if offset & bit:
            value = value + bit - 2 * bit * lax.rem(lax.div(index, bit), 2)
        bit *= 2
    return value


def find(pairs, block, wanted, what, rows):
    value = jnp.int32(0)
    valid = jnp.int32(0)
    for r in range(rows):
        hit = pairs[2, block, r] == wanted
        value = jnp.where(hit, what(r), value)
        valid = jnp.where(hit, jnp.int32(1), valid)
    return value, valid


LEVELS = 32766.0


def encode(values):
    size = jnp.abs(values)
    top = jnp.maximum(jnp.max(jnp.max(size, axis=0, keepdims=True), axis=1, keepdims=True), 1e-36)
    steps = (jnp.sqrt(size * (1.0 / top)) * LEVELS + 0.5).astype(jnp.int32)
    code = jnp.where(values < 0.0, -steps, steps).astype(jnp.int16)
    return code, jnp.broadcast_to(top, (1, LANES))


def decode(code, top):
    steps = code.astype(jnp.int32).astype(F32)
    return steps * jnp.abs(steps) * (top[:, 0:1] * (1.0 / (LEVELS * LEVELS)))


def exchange_kernel(
    pairs_in, offsets_in, orbitals_in, tables_in, small_in,
    landed, home, targets,
    pairs, offsets, orbitals, tables, small, sem_in,
    send_a, recv_a, slots_a, stage_i, stage_j, box_i, box_j, field, shifted, second,
    term_i, term_j, rows_i, every_i, rows_j, top_i, top_rows, every_top,
    send_d, recv_d, send_top, recv_top,
    sem_sa, sem_ra, sem_si, sem_ri, sem_sj, sem_rj, sem_st, sem_rt, sem_su, sem_ru, sem_sd, sem_rd,
    sem_sv, sem_rv, sem_sw, sem_rw,
):
    groups, cap, depth, cells = send_a.shape
    share, regions = box_i.shape[:2]
    rows = regions * share
    length = regions * depth
    local_count = orbitals.shape[0]
    me = lax.axis_index("orb")
    region = lax.axis_index("grp")
    grp_steps = range(regions)[:0:-1]
    order, needed, closed = slot_order(groups, cap, regions, rows)
    batches = range(share)
    begun = []

    def grp_peer(k):
        return partner(region, k)

    def other(n):
        return partner(me, order[n])

    loads = [
        pltpu.make_async_copy(source, target, sem_in.at[n])
        for n, (source, target) in enumerate((
            (pairs_in, pairs), (orbitals_in, orbitals), (offsets_in, offsets),
            (tables_in, tables), (small_in, small)))
    ]
    for load in loads[:2]:
        load.start()
    barrier = pltpu.get_barrier_semaphore()
    for k in range(1, groups):
        pl.semaphore_signal(
            barrier, inc=1, device_id={"orb": lax.rem(me + k, groups)}, device_id_type=MESH)
    for k in grp_steps:
        pl.semaphore_signal(barrier, inc=1, device_id={"grp": grp_peer(k)}, device_id_type=MESH)
    loads[0].wait()

    asked = []
    for n in range(groups):
        block = other(n)
        named = [(pairs[2, block, r] - me * cap, pairs[1, block, r]) for r in range(rows)]
        for c in range(cap):
            local = jnp.int32(0)
            for slot, place in named:
                local = jnp.where(slot == c, place, local)
            asked.append(local)
    loads[1].wait()
    for load in loads[2:]:
        load.start()
    for n in range(groups):
        for c in range(cap):
            send_a[n, c] = orbitals[asked[n * cap + c]]
    pl.semaphore_wait(barrier, groups + regions - 2)

    def orb_copy(peer, source, target, send_sem, recv_sem):
        return pltpu.make_async_remote_copy(
            src_ref=source, dst_ref=target, send_sem=send_sem, recv_sem=recv_sem,
            device_id={"orb": peer}, device_id_type=MESH)

    def pair_places(n):
        chip = order[n] // 2
        if chip == 0:
            return [(n, other(n))]
        core = lax.rem(me, 2)
        base = 2 * partner(lax.div(me, 2), chip)
        return [(n + 1 - core, base), (n + core, base + 1)]

    def bytes_of(ref, sem):
        return pltpu.make_async_copy(ref, ref, sem)

    def grp_send(source, target, send_sem, recv_sem):
        for k in grp_steps:
            peer = grp_peer(k)
            pltpu.make_async_remote_copy(
                src_ref=source.at[peer], dst_ref=target.at[region],
                send_sem=send_sem, recv_sem=recv_sem,
                device_id={"grp": peer}, device_id_type=MESH).start()
        begun.append(bytes_of(source.at[pl.ds(0, regions - 1)], send_sem))

    def grp_wait(source, target, send_sem, recv_sem):
        bytes_of(target.at[pl.ds(0, regions - 1)], recv_sem).wait()

    j_args = (stage_j, box_j, sem_sj.at[0], sem_rj.at[0])
    i_args = [(stage_i.at[b], box_i.at[b], sem_si.at[b], sem_ri.at[b]) for b in batches]
    t_args = [(term_i.at[b], rows_i[b], sem_st.at[b], sem_rt.at[b]) for b in batches]
    v_args = [(top_i.at[b], top_rows[b], sem_sv.at[b], sem_rv.at[b]) for b in batches]
    u_args = [(term_j.at[b], rows_j.at[b], sem_su.at[b], sem_ru.at[b]) for b in batches]

    spans = [range(needed[b - 1] if b else 0, needed[b]) for b in batches]

    for b in batches:
        for pair in spans[b][::2]:
            for n, peer in pair_places(pair):
                orb_copy(
                    peer, send_a.at[n], recv_a[b].at[n - spans[b][0]], sem_sa.at[0], sem_ra.at[b],
                ).start()
    begun.append(bytes_of(send_a.at[pl.ds(0, groups - 1)], sem_sa.at[0]))
    places = []
    for r in range(rows):
        slot = pairs[2, me, r]
        group = lax.div(slot, cap)
        place = jnp.int32(0)
        for n in range(groups):
            place = jnp.where(group == other(n), jnp.int32(n * cap), place)
        places.append(place + lax.rem(slot, cap))
    ranks = []
    for r in range(rows):
        rank = jnp.int32(0)
        for q in range(rows):
            if q != r:
                rank = rank + jnp.where(places[q] < places[r], jnp.int32(1), jnp.int32(0))
        ranks.append(rank)

    def ranked(values, rank):
        value = jnp.int32(0)
        for r in range(rows):
            value = jnp.where(ranks[r] == rank, values[r], value)
        return value

    row_of = [ranked([jnp.int32(r) for r in range(rows)], q) for q in range(rows)]
    place_of = [ranked(places, q) for q in range(rows)]
    rank_of = [
        find(pairs, me, other(n) * cap + c, lambda r: ranks[r], rows)[0]
        for n in range(groups) for c in range(cap)]

    for b in batches:
        for part in range(regions):
            stage_j[part, b] = orbitals[pairs[0, me, row_of[b * regions + part]]]
    grp_send(*j_args)
    for b in batches:
        for n in spans[b]:
            if not order[n]:
                for c in range(cap):
                    recv_a[b][n - spans[b][0], c] = send_a[n, c]
    box_j[region] = stage_j[region]

    for n in range(groups):
        for c in range(cap):
            local, valid = find(
                pairs, other(n), me * cap + c, lambda r: pairs[1, other(n), r], rows)
            targets[0, n * cap + c] = local
            targets[1, n * cap + c] = valid
    for r in range(rows):
        targets[2, r] = pairs[0, me, r]

    for load in loads[2:]:
        load.wait()
    sine = small[:, cells : cells + 3 * length].astype(BF16)
    green = small[:, :cells]

    row = lax.broadcasted_iota(jnp.int32, (length, cells), 0)
    col = lax.broadcasted_iota(jnp.int32, (length, cells), 1)
    mid = col // length
    last = col - mid * length
    lane = lax.broadcasted_iota(jnp.int32, (length, LANES), 1)
    inner = lax.rem(lane, length)
    near = inner < length // 2
    flip_y = LANES - length - lane + 2 * inner
    flip_z = lane + length - 1 - 2 * inner

    def shift(values, dx, dy, dz):
        moved = pltpu.roll(values, jnp.remainder(-dx + length, length), 0)
        flat = jnp.remainder(2 * cells - dy * length - dz, cells)
        moved = pltpu.roll(moved, flat, 1)
        x, y, z = row + dx, mid + dy, last + dz
        keep = (x >= 0) & (x < length) & (y >= 0) & (y < length) & (z >= 0) & (z < length)
        return jnp.where(keep, moved, 0.0)

    def taken(tile, index):
        return jnp.take_along_axis(tile, index, axis=1)

    def joined(tiles):
        return jnp.concatenate(tiles, axis=1)

    def folded(values):
        count = cells // LANES
        tiles = [values[:, n * LANES : (n + 1) * LANES] for n in range(count)]
        far = [taken(tiles[count - 1 - n], flip_y) for n in range(count // 2)]
        quarters = []
        for side in (1.0, -1.0):
            half = [tile + other if side > 0 else tile - other for tile, other in zip(tiles, far)]
            back = [taken(tile, flip_z) for tile in half]
            even = [tile + other for tile, other in zip(half, back)]
            odd = [tile - other for tile, other in zip(half, back)]
            for part in (even, odd):
                quarters.append(joined(
                    [jnp.where(near, part[n], part[n + 1]) for n in range(0, count // 2, 2)]))
        return quarters

    def unfolded(quarters):
        count = cells // LANES
        halves = []
        for even, odd in (quarters[:2], quarters[2:]):
            total, rest = even + odd, even - odd
            tiles = []
            for n in range(count // 4):
                here = slice(n * LANES, (n + 1) * LANES)
                tiles.append(jnp.where(near, total[:, here], taken(rest[:, here], flip_z)))
                tiles.append(jnp.where(near, taken(total[:, here], flip_z), rest[:, here]))
            halves.append(tiles)
        first = [even + odd for even, odd in zip(*halves)]
        return joined(first + [taken(even - odd, flip_y) for even, odd in zip(*halves)][::-1])

    def product(values, n):
        count = values.shape[0]
        high, low = split_field(values)
        both = dot(jnp.concatenate([high, low], axis=0), tables[2 * n])
        return both[:count] + both[count:] + dot(high, tables[2 * n + 1])

    def along_x(values):
        high, low = split_field(values)
        return dot(sine, jnp.concatenate([high, low, high], axis=0))

    def whole(box, b):
        for part in range(regions):
            field[b, part * depth : (part + 1) * depth, :] = box(part).astype(F32)
        return field[b]

    moves = []
    for b in batches:
        r = jnp.int32(0)
        for part in range(regions):
            r = jnp.where(region == part, row_of[b * regions + part], r)
        j = me * local_count + pairs[0, me, r]
        i = lax.div(pairs[2, me, r], cap) * local_count + pairs[1, me, r]
        moves.append([offsets[a, j] - offsets[a, i] for a in range(3)])

    grp_wait(*j_args)
    for b in batches:
        shifted[b] = shift(whole(lambda part: box_j[part, b], b), *moves[b])

    for b in batches:
        away = sum(order[n] > 0 for n in spans[b])
        bytes_of(recv_a[b].at[pl.ds(0, away)], sem_ra.at[b]).wait()
        if b:
            for n in spans[b]:
                for c in range(cap):
                    slots_a[b][n * cap + c] = recv_a[b][n - spans[b][0], c]
        for part in range(regions):
            place = jnp.minimum(place_of[b * regions + part], needed[b] * cap - 1)
            if b:
                stage_i[b, part] = slots_a[b][place]
            else:
                stage_i[b, part] = recv_a[b][lax.div(place, cap), lax.rem(place, cap)]
        grp_send(*i_args[b])
        box_i[b, region] = stage_i[b, region]
        if b + 1 < share:
            for n in range(needed[b] * cap):
                slots_a[b + 1][n] = slots_a[b][n] if b else recv_a[b][n // cap, n % cap]

    quarter = cells // 4
    for b in batches:
        grp_wait(*i_args[b])
        second[b] = whole(lambda part: box_i[b, part], b)
        charge = second[b] * shifted[b]
        spectrum = joined([product(part, 2 * q) for q, part in enumerate(folded(charge))])
        spectrum = along_x(along_x(spectrum) * green)
        field[b] = unfolded([
            product(spectrum[:, q * quarter : (q + 1) * quarter], 2 * q + 1) for q in range(4)])
        code, top = encode(field[b] * shifted[b])
        for part in range(regions):
            term_i[b, part] = code[part * depth : (part + 1) * depth, :]
            top_i[b, part] = top
        grp_send(*t_args[b])
        grp_send(*v_args[b])
        rows_i[b][region] = term_i[b, region]
        top_rows[b][region] = top_i[b, region]

    for b in batches:
        term = shift(field[b] * second[b], *[-d for d in moves[b]])
        for part in range(regions):
            term_j[b, part] = term[part * depth : (part + 1) * depth, :]
        rows_j[b, region] = term_j[b, region]

    sends = []
    for b in batches:
        grp_wait(*t_args[b])
        grp_wait(*v_args[b])
        if b:
            for part in range(regions):
                every_i[b][b * regions + part] = rows_i[b][part]
                every_top[b][b * regions + part] = top_rows[b][part]
        leaving = range(closed[b - 1] if b else 0, closed[b])
        for n in leaving:
            for c in range(cap):
                q = jnp.minimum(rank_of[n * cap + c], (b + 1) * regions - 1)
                send_d[n, c] = every_i[b][q] if b else rows_i[b][q]
                send_top[n, c : c + 1] = every_top[b][q] if b else top_rows[b][q]
        pairs_leaving = sorted(leaving[::2], key=lambda n: -order[n])
        for pair in pairs_leaving:
            for n, peer in pair_places(pair):
                orb_copy(
                    peer, send_top.at[n], recv_top.at[n], sem_sw.at[0], sem_rw.at[b]).start()
                orb_copy(
                    peer, send_d.at[n], recv_d.at[n], sem_sd.at[0], sem_rd.at[pair // 2]).start()
        sends.append(pairs_leaving)
        for later in range(b + 1, share):
            for part in range(regions):
                every_i[later][b * regions + part] = rows_i[b][part]
                every_top[later][b * regions + part] = top_rows[b][part]
        if b == 0:
            for args in u_args:
                grp_send(*args)

    def arrived(n, codes, tops):
        for c in range(cap):
            landed[n, c] = decode(codes[n, c], tops[n, c : c + 1])

    for n in range(groups):
        if not order[n]:
            arrived(n, send_d, send_top)
    for args in u_args:
        grp_wait(*args)
    for r in range(rows):
        home[r] = rows_j[lax.div(ranks[r], regions), lax.rem(ranks[r], regions)]
    for b in batches:
        away = [[n for n in (pair, pair + 1) if order[n]] for pair in sends[b]]
        bytes_of(recv_top.at[pl.ds(0, sum(map(len, away)))], sem_rw.at[b]).wait()
        for pair, both in zip(sends[b], away):
            bytes_of(recv_d.at[pl.ds(pair, len(both))], sem_rd.at[pair // 2]).wait()
            for n in both:
                arrived(n, recv_d, recv_top)
    begun.append(bytes_of(send_top.at[pl.ds(0, groups - 1)], sem_sw.at[0]))
    begun.append(bytes_of(send_d.at[pl.ds(0, groups - 1)], sem_sd.at[0]))
    for copy in begun:
        copy.wait()


def exchange_terms(pairs, offsets, orbitals, groups, regions):
    _, depth, cells = orbitals.shape
    rows = pairs.shape[2]
    share = rows // regions
    cap = 2 * rows // groups
    length = depth * regions
    vmem = pl.BlockSpec(memory_space=pltpu.VMEM)
    operands = (pairs, offsets, orbitals, *[jnp.asarray(t) for t in fixed_tables(length)])
    spaces = [pltpu.SMEM, pltpu.SMEM] + [pltpu.VMEM] * 3
    by_slot = (groups, cap, depth, cells)
    by_batch = (share, regions, depth, cells)
    by_region = (regions, depth, cells)
    dma = pltpu.SemaphoreType.DMA
    one, each, orb_sem = dma((1,)), dma((share,)), dma((groups // 2,))
    _, needed, _ = slot_order(groups, cap, regions, rows)
    parts = [last - first for first, last in zip([0] + needed[:-1], needed)]
    box = (length, cells)
    i16 = jnp.int16
    return pl.pallas_call(
        exchange_kernel,
        out_shape=(
            jax.ShapeDtypeStruct(by_slot, F32), jax.ShapeDtypeStruct((rows, depth, cells), F32),
            pltpu.SMEM((3, groups * cap), jnp.int32)),
        in_specs=[pl.BlockSpec(memory_space=pltpu.HBM)] * len(operands),
        out_specs=(vmem, vmem, pl.BlockSpec(memory_space=pltpu.SMEM)),
        scratch_shapes=[
            *[space(x.shape, x.dtype) for space, x in zip(spaces, operands)],
            dma((len(operands),)),
            pltpu.VMEM(by_slot, BF16),
            [pltpu.VMEM((count, cap, depth, cells), BF16) for count in parts],
            [pltpu.VMEM((count * cap, depth, cells), BF16) for count in needed],
            pltpu.VMEM(by_batch, BF16),
            pltpu.VMEM((regions, share, depth, cells), BF16),
            pltpu.VMEM(by_batch, BF16),
            pltpu.VMEM((regions, share, depth, cells), BF16),
            pltpu.VMEM((share, *box), F32), pltpu.VMEM((share, *box), F32),
            pltpu.VMEM((share, *box), F32),
            pltpu.VMEM(by_batch, i16), pltpu.VMEM(by_batch, F32),
            [pltpu.VMEM(by_region, i16) for _ in range(share)],
            [pltpu.VMEM(((b + 1) * regions, depth, cells), i16) for b in range(share)],
            pltpu.VMEM(by_batch, F32),
            pltpu.VMEM((share, regions, 1, LANES), F32),
            [pltpu.VMEM((regions, 1, LANES), F32) for _ in range(share)],
            [pltpu.VMEM(((b + 1) * regions, 1, LANES), F32) for b in range(share)],
            pltpu.VMEM(by_slot, i16), pltpu.VMEM(by_slot, i16),
            pltpu.VMEM((groups, cap, LANES), F32), pltpu.VMEM((groups, cap, LANES), F32),
            one, each, each, each, one, one, each, each, each, each, one, orb_sem,
            each, each, one, each,
        ],
        compiler_params=pltpu.CompilerParams(
            collective_id=0, has_side_effects=True, vmem_limit_bytes=32 * 1024 * 1024),
    )(*[pltpu.with_memory_space_constraint(x, pltpu.HBM) for x in operands])


def collect_kernel(landed, home, targets, out):
    groups, cap = landed.shape[:2]
    out[...] = jnp.zeros_like(out)
    for r in range(home.shape[0]):
        out[targets[2, r]] += home[r]
    for n in range(groups):
        for c in range(cap):
            slot = n * cap + c
            out[targets[0, slot]] += jnp.where(targets[1, slot] > 0, landed[n, c], 0.0)


def collect(landed, home, targets, shape):
    vmem = pl.BlockSpec(memory_space=pltpu.VMEM)
    return pl.pallas_call(
        collect_kernel,
        out_shape=jax.ShapeDtypeStruct(shape, F32),
        in_specs=[vmem, vmem, pl.BlockSpec(memory_space=pltpu.SMEM)],
        out_specs=vmem,
        compiler_params=pltpu.CompilerParams(vmem_limit_bytes=32 * 1024 * 1024),
    )(landed, home, pltpu.with_memory_space_constraint(targets, pltpu.SMEM))


def per_device(orbitals, pair_list, offsets):
    groups = lax.axis_size("orb")
    regions = lax.axis_size("grp")
    pairs = jnp.transpose(pair_list, (2, 0, 1))
    landed, home, targets = exchange_terms(pairs, offsets.T, orbitals, groups, regions)
    return collect(landed, home, targets, orbitals.shape)


def solution(mesh):
    in_specs = (P("orb", "grp", None), P(), P())
    out_specs = P("orb", "grp", None)
    return jax.shard_map(
        per_device, mesh=mesh, in_specs=in_specs, out_specs=out_specs, check_vma=False
    )
```
